32 devices in a mesh: grp: 4 (over z), pen: 8 (over y, x, core).
Axes of the slice: x: 2, y: 2, z: 4, core: 2. Of those that a mesh axis runs over, the one named last changes fastest.
Arguments:
- cell_offsets: int32 [2, 1048576], P(None, ('grp', 'pen')), may hold values from 0 to 1
- cell_z: int32 [1048576], P(('grp', 'pen')), may hold values from 0 to 255
- frac: float32 [3, 1048576], P(None, ('grp', 'pen')), may hold values from 0 to 1
- charges: float32 [1048576], P(('grp', 'pen')), may hold values from -4 to 4
- tile_counts: int32 [16384], P(('grp', 'pen')), may hold values from 16 to 64, as said below
Outputs:
- forces: float32 [3, 1048576], P(None, ('grp', 'pen'))
- energy: float32 [], replicated
The draws below stay inside these ranges and needn't reach their ends.
Inputs may be any that keep to these rules, and one draw needn't show every extreme that they name: `tile_counts`: live slots of each tile; some tile holds 64.
All inputs are finite; a program needn't handle non-finite values.
Results may differ from the reference program's by a relative error of at most 0.0003.
Values sent between devices are 32-bit elements; how exact they have to be, the bound alone decides.
No kernel may reach another device: no remote copies, remote signals or barrier semaphores. Data moves between devices by JAX's collectives and lax.ppermute only.
A program may use at most 256 MiB of HBM per device.

```python
import math
import jax
import jax.numpy as jnp
from jax import lax

KX = 256
KY = 256
KZ = 256
SLOTS = 64
TILES = 16384
ATOMS = 1048576
N_GRP = 4
N_PEN = 8


def draw_tile_counts(key, part):
    counts = jax.random.randint(key, (TILES,), max(1, SLOTS // 4), SLOTS + 1)
    filled = jax.random.randint(jax.random.fold_in(key, 7), (), 0, TILES)
    return counts.at[filled].set(SLOTS).astype(jnp.int32)


def place_ends(drawn, key, low, top_value):
    dims = drawn.shape
    spot = [jax.random.randint(jax.random.fold_in(key, axis), (), 0, dims[axis]) for axis in range(len(dims))]
    drawn = drawn.at[tuple(spot)].set(low)
    longest = dims.index(max(dims))
    spot[longest] = (spot[longest] + 1) % dims[longest]
    return drawn.at[tuple(spot)].set(top_value)


def steps_of(own_key, shape, cuts, least, high):
    gain, own = 1.0, jax.random.fold_in(own_key, 6)
    for axis_at, shards_of in cuts:
        steps = jnp.exp(jax.random.uniform(jax.random.fold_in(own, axis_at), (shards_of,), jnp.float32, least / len(cuts), high / len(cuts)))
        gain = gain * jnp.repeat(steps, shape[axis_at] // shards_of).reshape([-1 if axis == axis_at else 1 for axis in range(len(shape))])
    return gain


def scatter_about(stream_key, shape, width, limit, shards=(), kind=jnp.bfloat16):
    array = jax.random.normal(stream_key, shape, jnp.float32) * width
    if len(shards) > 0:
        array = steps_of(stream_key, shape, shards, -0.22, 0.18) * array
    return jnp.clip(array, min=-limit, max=limit).astype(kind)


def setup_inputs(seed: int = 0) -> dict:
    arg_keys = jax.random.split(jax.random.key(seed), 6)
    return {
        "cell_offsets": place_ends(jax.random.randint(arg_keys[0], (2, ATOMS), 0, 2), jax.random.fold_in(arg_keys[0], 1), 0, 1).astype(jnp.int32),
        "cell_z": place_ends(jax.random.randint(arg_keys[1], (ATOMS,), 0, KZ), jax.random.fold_in(arg_keys[1], 1), 0, KZ - 1).astype(jnp.int32),
        "frac": jnp.clip(1.0 * jax.random.uniform(arg_keys[2], (3, ATOMS), jnp.float32) ** steps_of(arg_keys[2], (3, ATOMS), ((1, 32),), -0.2, 0.2), 0.0, 1.0),
        "charges": scatter_about(arg_keys[3], (ATOMS,), 1.0, 4.0, ((0, 32),), jnp.float32),
        "tile_counts": draw_tile_counts(jax.random.fold_in(arg_keys[5], 71), 0),
    }


ewald_split = 0.6


def spline_rows(fracs):
    values = [jnp.ones_like(fracs)]
    fifth = values
    for order in range(2, 7):
        nxt = []
        for j in range(order):
            term = jnp.zeros_like(fracs)
            if j >= 1:
                term = term + values[j - 1] * (fracs + order - 1 - j)
            if j <= order - 2:
                term = term + values[j] * (1.0 - fracs + j)
            nxt.append(term / (order - 1))
        if order == 5:
            fifth = nxt
        values = nxt
    slopes = []
    for j in range(6):
        term = jnp.zeros_like(fracs)
        if j >= 1:
            term = term + fifth[j - 1]
        if j <= 4:
            term = term - fifth[j]
        slopes.append(term)
    return values, slopes


def tile_weights(offsets, zcell, fracs, charge, counts, size_z):
    slots = charge.shape[-1]
    live = (jnp.arange(slots, dtype=jnp.int32) < counts[..., None]).astype(jnp.float32)
    live_q = charge * live
    theta_x, slope_x = spline_rows(fracs[0])
    theta_y, slope_y = spline_rows(fracs[1])
    theta_z, slope_z = spline_rows(fracs[2])
    footing = jnp.arange(8, dtype=jnp.int32)[:, None]
    cells = jnp.arange(size_z, dtype=jnp.int32)
    weight_x = 0.0
    grade_x = 0.0
    weight_y = 0.0
    grade_y = 0.0
    weight_z = 0.0
    grade_z = 0.0
    for j in range(6):
        hit_x = (footing == offsets[0][..., None, :] + j).astype(jnp.float32)
        hit_y = (footing == offsets[1][..., None, :] + j).astype(jnp.float32)
        hit_z = (cells == (zcell[..., :, None] + j) % size_z).astype(jnp.float32)
        weight_x = weight_x + theta_x[j][..., None, :] * hit_x
        grade_x = grade_x + slope_x[j][..., None, :] * hit_x
        weight_y = weight_y + theta_y[j][..., None, :] * hit_y
        grade_y = grade_y + slope_y[j][..., None, :] * hit_y
        weight_z = weight_z + theta_z[j][..., :, None] * hit_z
        grade_z = grade_z + slope_z[j][..., :, None] * hit_z
    return weight_x, grade_x, weight_y, grade_y, weight_z, grade_z, live_q


def modulus(index, length):
    coeffs = (1.0 / 120.0, 26.0 / 120.0, 66.0 / 120.0, 26.0 / 120.0, 1.0 / 120.0)
    real_part = 0.0
    imag_part = 0.0
    for j in range(5):
        angle = ((index * j) % length).astype(jnp.float32) * (2.0 * math.pi / length)
        real_part = real_part + coeffs[j] * jnp.cos(angle)
        imag_part = imag_part + coeffs[j] * jnp.sin(angle)
    return real_part * real_part + imag_part * imag_part


def influence(index_x, index_y, index_z):
    freq_x = jnp.where(2 * index_x < KX, index_x, index_x - KX).astype(jnp.float32) / KX
    freq_y = jnp.where(2 * index_y < KY, index_y, index_y - KY).astype(jnp.float32) / KY
    freq_z = jnp.where(2 * index_z < KZ, index_z, index_z - KZ).astype(jnp.float32) / KZ
    square = freq_x * freq_x + freq_y * freq_y + freq_z * freq_z
    safe = jnp.where(square > 0, square, 1.0)
    volume = float(KX * KY * KZ)
    value = jnp.exp(-(math.pi ** 2) * safe / (ewald_split ** 2)) / (math.pi * volume * safe)
    value = value / (modulus(index_x, KX) * modulus(index_y, KY) * modulus(index_z, KZ))
    return jnp.where(square > 0, value, 0.0)


def reference(cell_offsets, cell_z, frac, charges, tile_counts):
    tiles_x = KX // N_GRP // 2
    tiles_y = KY // N_PEN // 2
    rows_x = KX // 2
    rows_y = KY // 2
    highest = lax.Precision.HIGHEST

    def arrange(arr):
        lead = arr.shape[:-1]
        count = len(lead)
        shaped = arr.reshape(lead + (N_GRP, N_PEN, tiles_x, tiles_y, SLOTS))
        order = tuple(range(count)) + (count, count + 2, count + 1, count + 3, count + 4)
        return jnp.transpose(shaped, order).reshape(lead + (rows_x, rows_y, SLOTS))

    offsets = jnp.moveaxis(arrange(cell_offsets), 1, 0)
    fracs = jnp.moveaxis(arrange(frac), 1, 0)
    zcell = arrange(cell_z)
    charge = arrange(charges)
    counts = jnp.transpose(tile_counts.reshape(N_GRP, N_PEN, tiles_x, tiles_y), (0, 2, 1, 3)).reshape(rows_x, rows_y)
    row_ids = jnp.arange(rows_x, dtype=jnp.int32)
    eight = jnp.arange(8, dtype=jnp.int32)

    def spread_row(grid, inputs):
        offs, zrow, frow, qrow, crow, row = inputs
        weight_x, grade_x, weight_y, grade_y, weight_z, grade_z, live_q = tile_weights(offs, zrow, frow, qrow, crow, KZ)
        pair = (weight_x[:, :, None, :] * weight_y[:, None, :, :] * live_q[:, None, None, :]).reshape(rows_y, 64, SLOTS)
        spread = jnp.einsum("tfs,tsz->tfz", pair, weight_z, precision=highest).reshape(rows_y, 8, 4, 2, KZ)
        slab = 0.0
        for j in range(4):
            part = jnp.transpose(spread[:, :, j], (1, 0, 2, 3))
            slab = slab + jnp.roll(part, j, axis=1).reshape(8, KY, KZ)
        targets = (2 * row + eight) % KX
        return grid.at[targets].add(slab), None

    start = jnp.zeros((KX, KY, KZ), jnp.float32)
    charge_mesh, _ = lax.scan(spread_row, start, (offsets, zcell, fracs, charge, counts, row_ids))
    spectrum = jnp.fft.fftn(charge_mesh)
    index_x = jnp.arange(KX, dtype=jnp.int32)[:, None, None]
    index_y = jnp.arange(KY, dtype=jnp.int32)[None, :, None]
    index_z = jnp.arange(KZ, dtype=jnp.int32)[None, None, :]
    kernel = influence(index_x, index_y, index_z)
    power = jnp.real(spectrum) ** 2 + jnp.imag(spectrum) ** 2
    energy = 0.5 * jnp.sum(kernel * power)
    potential = jnp.real(jnp.fft.ifftn(kernel * spectrum)) * float(KX * KY * KZ)

    def interp_row(carry, inputs):
        offs, zrow, frow, qrow, crow, row = inputs
        weight_x, grade_x, weight_y, grade_y, weight_z, grade_z, live_q = tile_weights(offs, zrow, frow, qrow, crow, KZ)
        rows = jnp.take(potential, (2 * row + eight) % KX, axis=0)
        parts = []
        for j in range(4):
            parts.append(jnp.roll(rows, -2 * j, axis=1).reshape(8, rows_y, 2, KZ))
        footing = jnp.transpose(jnp.stack(parts, axis=0), (2, 1, 0, 3, 4)).reshape(rows_y, 64, KZ)
        main = jnp.einsum("tfz,tsz->tfs", footing, weight_z, precision=highest).reshape(rows_y, 8, 8, SLOTS)
        tilt = jnp.einsum("tfz,tsz->tfs", footing, grade_z, precision=highest).reshape(rows_y, 8, 8, SLOTS)
        force_x = -live_q * jnp.einsum("txs,tys,txys->ts", grade_x, weight_y, main, precision=highest)
        force_y = -live_q * jnp.einsum("txs,tys,txys->ts", weight_x, grade_y, main, precision=highest)
        force_z = -live_q * jnp.einsum("txs,tys,txys->ts", weight_x, weight_y, tilt, precision=highest)
        return carry, jnp.stack([force_x, force_y, force_z], axis=0)

    _, stacked = lax.scan(interp_row, 0.0, (offsets, zcell, fracs, charge, counts, row_ids))
    forces = stacked.reshape(N_GRP, tiles_x, 3, N_PEN, tiles_y, SLOTS)
    forces = jnp.transpose(forces, (2, 0, 3, 1, 4, 5)).reshape(3, ATOMS)
    return forces, (energy / ATOMS).astype(jnp.float32)
```

```python
import math

import jax
import jax.numpy as jnp
import numpy as np
from jax import lax
from jax.experimental import pallas as pl
from jax.experimental.pallas import tpu as pltpu
from jax.sharding import PartitionSpec as P

KX = 256
KY = 256
KZ = 256
LANES = 128
ROWS = 16
SPAN = 7
REACH = 5

ewald_split = 0.6
highest = lax.Precision.HIGHEST
f32 = jnp.float32
bf16 = jnp.bfloat16


def shifted(block, axis, distance):
    devices = range(lax.axis_size(axis))
    route = [((i - distance) % len(devices), i) for i in devices]
    return lax.ppermute(block, axis, route)


def shifted_both(block, distance):
    groups, pens = lax.axis_size("grp"), lax.axis_size("pen")
    route = []
    for g in range(groups):
        for p in range(pens):
            source = ((g - distance) % groups) * pens + (p - distance) % pens
            route.append((source, g * pens + p))
    return lax.ppermute(block, ("grp", "pen"), route)


def halves(value):
    high = value.astype(bf16)
    low = (value - high.astype(f32)).astype(bf16)
    return high, low


def table_halves(table):
    table = jnp.asarray(np.asarray(table, np.float32))
    return halves(table)


def dot(left, right, dims):
    return lax.dot_general(left, right, (dims, ((), ())), preferred_element_type=f32)


NN = ((1,), (0,))
NT = ((1,), (1,))


def spline_rows(x):
    values = [jnp.ones_like(x)]
    fifth = None
    for order in range(2, 7):
        nxt = []
        for j in range(order):
            term = None
            if j >= 1:
                term = values[j - 1] * (x + float(order - 1 - j))
            if j <= order - 2:
                other = values[j] * (float(1 + j) - x)
                term = other if term is None else term + other
            nxt.append(term)
        if order == 5:
            fifth = [v * (1.0 / 24.0) for v in nxt]
        values = nxt
    thetas = [v * (1.0 / 120.0) for v in values]
    slopes = [-fifth[0]]
    for j in range(1, 5):
        slopes.append(fifth[j - 1] - fifth[j])
    slopes.append(fifth[4])
    return thetas, slopes


def placed(rows, offset):
    out = []
    zero = jnp.zeros_like(rows[0])
    for i in range(SPAN):
        here = rows[i] if i <= 5 else zero
        before = rows[i - 1] if i >= 1 else zero
        out.append(jnp.where(offset == 0, here, before))
    return out


def spread_out(row):
    return jnp.broadcast_to(row, (ROWS, row.shape[-1]))


def live_charges(q_ref, counts_ref, step, slots):
    per_row = LANES // slots
    row_at = lax.broadcasted_iota(jnp.int32, (8, LANES), 0)
    lane_at = lax.broadcasted_iota(jnp.int32, (8, LANES), 1)
    tile_at = row_at * per_row + lane_at // slots
    count = jnp.zeros((8, LANES), jnp.int32)
    for k in range(8 * per_row):
        count = jnp.where(tile_at == k, counts_ref[step * (8 * per_row) + k], count)
    charge = q_ref[pl.ds(pl.multiple_of(step * 8, 8), 8), :]
    return jnp.where(lane_at % slots < count, charge, 0.0)


def step_rows(step, frac_ref, offs_ref, z_ref, slots):
    rows = pl.ds(pl.multiple_of(step * 8, 8), 8)
    fracs = [frac_ref[d, rows, :] for d in range(3)]
    offset_x = offs_ref[0, rows, :]
    offset_y = offs_ref[1, rows, :]
    row_at = lax.broadcasted_iota(jnp.int32, (8, LANES), 0)
    lane_at = lax.broadcasted_iota(jnp.int32, (8, LANES), 1)
    per_row = LANES // slots
    tile_in_group = (row_at % 2) * per_row + lane_at // slots
    offset_y = offset_y + 2 * tile_in_group
    return fracs, offset_x, offset_y, z_ref[rows, :]


def by_distance(distance, rows, row):
    out = jnp.where(distance == 0, spread_out(rows[0][row]), 0.0)
    for j in range(1, 6):
        out = jnp.where(distance == j, spread_out(rows[j][row]), out)
    return out


def z_parts(zcell, row, lists):
    cell = spread_out(zcell[row])
    at = lax.broadcasted_iota(jnp.int32, (ROWS, LANES), 0)
    ahead = (at - cell) & (ROWS - 1)
    block = ((cell + ahead) & (KZ - 1)) // ROWS
    weights = [by_distance(ahead, rows, row) for rows in lists]
    return block.astype(f32).astype(bf16), weights


def z_matrix(block, weight):
    zero = jnp.zeros_like(weight)
    return jnp.concatenate(
        [jnp.where(block == jnp.array(k, bf16), weight, zero) for k in range(KZ // ROWS)], axis=0
    )


def group_place(step, k, groups):
    index = step * 4 + k
    return index // groups, index % groups


def spread_body(
    counts_ref, frac_ref, offs_ref, z_ref, q_ref, core_ref, rim_y_ref, rim_x_ref, corner_ref, acc_ref,
    *, slots, groups, block_x, block_y,
):
    acc_ref[...] = jnp.zeros_like(acc_ref)
    at = lax.broadcasted_iota(jnp.int32, (ROWS, LANES), 0)

    def body(step, carry):
        fracs, offset_x, offset_y, zcell = step_rows(step, frac_ref, offs_ref, z_ref, slots)
        charge = live_charges(q_ref, counts_ref, step, slots)
        theta_x, _ = spline_rows(fracs[0])
        theta_y, _ = spline_rows(fracs[1])
        theta_z, _ = spline_rows(fracs[2])
        theta_y = [t * charge for t in theta_y]
        weight_x = placed(theta_x, offset_x)
        for k in range(4):
            blocks, zs, pairs = [], [], []
            for half in range(2):
                row = slice(2 * k + half, 2 * k + half + 1)
                block, (weight,) = z_parts(zcell, row, [theta_z])
                blocks.append(block)
                zs.append(weight)
                weight_y = by_distance(at - spread_out(offset_y[row]), theta_y, row)
                pairs.append([spread_out(weight_x[i][row]) * weight_y for i in range(SPAN)])
            block = jnp.concatenate(blocks, axis=1)
            z_high, z_low = halves(jnp.concatenate(zs, axis=1))
            table_high = z_matrix(block, z_high)
            table_low = z_matrix(block, z_low)
            pair = jnp.concatenate(
                [jnp.concatenate([pairs[0][i], pairs[1][i]], axis=1) for i in range(SPAN)], axis=0
            )
            high, low = halves(pair)
            both = dot(jnp.concatenate([high, low], axis=0), table_high, NT)
            rest = dot(high, table_low, NT)
            total = both[: SPAN * ROWS] + both[SPAN * ROWS :] + rest
            a, g = group_place(step, k, groups)
            where = (pl.ds(2 * a, SPAN), pl.ds(pl.multiple_of(8 * g, 8), ROWS))
            acc_ref[where[0], where[1], :] += total.reshape(SPAN, ROWS, KZ)
        return carry

    lax.fori_loop(0, frac_ref.shape[1] // 8, body, 0)
    core_ref[...] = acc_ref[:block_x, :block_y, :]
    rim_y_ref[...] = acc_ref[:block_x, block_y : block_y + 8, :]
    rim_x_ref[...] = acc_ref[block_x : block_x + REACH, :block_y, :]
    corner_ref[...] = acc_ref[block_x : block_x + REACH, block_y : block_y + 8, :]


vmem = pl.BlockSpec(memory_space=pltpu.VMEM)
smem = pl.BlockSpec(memory_space=pltpu.SMEM)


def spread_charges(counts, frac, offs, zcell, charge, slots, groups, block_x, block_y):
    import functools

    body = functools.partial(spread_body, slots=slots, groups=groups, block_x=block_x, block_y=block_y)
    shapes = [
        (block_x, block_y, KZ), (block_x, 8, KZ), (REACH, block_y, KZ), (REACH, 8, KZ),
    ]
    return pl.pallas_call(
        body,
        out_shape=[jax.ShapeDtypeStruct(s, f32) for s in shapes],
        in_specs=[smem] + [vmem] * 4,
        out_specs=[vmem] * 4,
        scratch_shapes=[pltpu.VMEM((block_x + REACH, block_y + 8, KZ), f32)],
        name="spread",
    )(counts, frac, offs, zcell, charge)


def interp_body(
    counts_ref, frac_ref, offs_ref, z_ref, q_ref, core_ref, rim_y_ref, rim_x_ref, corner_ref, out_ref, pot_ref,
    *, slots, groups, block_x, block_y,
):
    pot_ref[:block_x, :block_y, :] = core_ref[...]
    pot_ref[:block_x, block_y : block_y + 8, :] = rim_y_ref[...]
    pot_ref[block_x : block_x + REACH, :block_y, :] = rim_x_ref[...]
    pot_ref[block_x : block_x + REACH, block_y : block_y + 8, :] = corner_ref[...]
    at = lax.broadcasted_iota(jnp.int32, (ROWS, LANES), 0)
    height = SPAN * ROWS

    def body(step, carry):
        fracs, offset_x, offset_y, zcell = step_rows(step, frac_ref, offs_ref, z_ref, slots)
        charge = live_charges(q_ref, counts_ref, step, slots)
        theta_x, slope_x = spline_rows(fracs[0])
        theta_y, slope_y = spline_rows(fracs[1])
        theta_z, slope_z = spline_rows(fracs[2])
        theta_y = [t * -charge for t in theta_y]
        slope_y = [t * -charge for t in slope_y]
        weight_x = placed(theta_x, offset_x)
        grade_x = placed(slope_x, offset_x)
        rows_out = [[], [], []]
        for k in range(4):
            blocks, zs, gs = [], [], []
            for half in range(2):
                row = slice(2 * k + half, 2 * k + half + 1)
                block, (weight, grade) = z_parts(zcell, row, [theta_z, slope_z])
                blocks.append(block)
                zs.append(weight)
                gs.append(grade)
            block = jnp.concatenate(blocks, axis=1)
            z_high, z_low = halves(jnp.concatenate(zs, axis=1))
            g_high, g_low = halves(jnp.concatenate(gs, axis=1))
            a, g = group_place(step, k, groups)
            slab = pot_ref[pl.ds(2 * a, SPAN), pl.ds(pl.multiple_of(8 * g, 8), ROWS), :]
            high, low = halves(slab.reshape(height, KZ))
            stacked = jnp.concatenate([high, low], axis=0)
            main = dot(stacked, z_matrix(block, z_high), NN)
            main = main[:height] + main[height:] + dot(high, z_matrix(block, z_low), NN)
            tilt = dot(stacked, z_matrix(block, g_high), NN)
            tilt = tilt[:height] + tilt[height:] + dot(high, z_matrix(block, g_low), NN)
            for half in range(2):
                row = slice(2 * k + half, 2 * k + half + 1)
                lanes = slice(half * LANES, (half + 1) * LANES)
                away = at - spread_out(offset_y[row])
                weight_y = by_distance(away, theta_y, row)
                grade_y = by_distance(away, slope_y, row)
                plain = steep = tilted = 0.0
                for i in range(SPAN):
                    part = slice(i * ROWS, (i + 1) * ROWS)
                    wide = spread_out(weight_x[i][row])
                    plain = plain + wide * main[part, lanes]
                    tilted = tilted + wide * tilt[part, lanes]
                    steep = steep + spread_out(grade_x[i][row]) * main[part, lanes]
                rows_out[0].append(jnp.sum(steep * weight_y, axis=0, keepdims=True))
                rows_out[1].append(jnp.sum(plain * grade_y, axis=0, keepdims=True))
                rows_out[2].append(jnp.sum(tilted * weight_y, axis=0, keepdims=True))
        for d in range(3):
            out_ref[d, pl.ds(pl.multiple_of(step * 8, 8), 8), :] = jnp.concatenate(rows_out[d], axis=0)
        return carry

    lax.fori_loop(0, frac_ref.shape[1] // 8, body, 0)


def interpolate(counts, frac, offs, zcell, charge, core, rims, slots, groups, block_x, block_y):
    import functools

    body = functools.partial(interp_body, slots=slots, groups=groups, block_x=block_x, block_y=block_y)
    return pl.pallas_call(
        body,
        out_shape=jax.ShapeDtypeStruct(frac.shape, f32),
        in_specs=[smem] + [vmem] * 8,
        out_specs=vmem,
        scratch_shapes=[pltpu.VMEM((block_x + REACH, block_y + 8, KZ), f32)],
        name="interpolate",
    )(counts, frac, offs, zcell, charge, core, *rims)


def angles(left, right, length):
    return (np.outer(left, right) % length) * (2.0 * math.pi / length)


def np_modulus(length):
    index = np.arange(length)
    coeffs = (1.0 / 120.0, 26.0 / 120.0, 66.0 / 120.0, 26.0 / 120.0, 1.0 / 120.0)
    total = 0.0
    for j in range(5):
        total = total + coeffs[j] * np.exp(2j * math.pi * ((index * j) % length) / length)
    return np.abs(total) ** 2


def np_line(length):
    index = np.arange(length)
    freq = np.where(2 * index < length, index, index - length) / length
    square = freq * freq
    return square, np.exp(-(math.pi**2) * square / ewald_split**2) / np_modulus(length)


def z_table(devices):
    per = KZ // 2 // devices
    position = np.arange(KZ)
    forward, back = [], []
    for device in range(devices):
        for imaginary in range(2):
            for plane in range(device * per, (device + 1) * per):
                wave = 2.0 * math.pi * ((plane * position) % KZ) / KZ
                if plane == 0:
                    row = np.where(position % 2 == 0, 1.0, -1.0) if imaginary else np.ones(KZ)
                    forward.append(row)
                    back.append(row)
                else:
                    row = -np.sin(wave) if imaginary else np.cos(wave)
                    forward.append(row)
                    back.append(2.0 * row)
    return np.stack(forward), np.stack(back)


def forward_z_body(core_ref, rim_y_ref, rim_x_ref, corner_ref, high_ref, low_ref, out_ref, *, chunk):
    block_x, block_y = core_ref.shape[:2]
    high = high_ref[...]
    low = low_ref[...]
    stacked = jnp.concatenate([high, low], axis=0)
    size = high.shape[0]
    for start in range(0, block_x, chunk):
        part = core_ref[start : start + chunk]
        edge = part[:, :8] + rim_y_ref[start : start + chunk]
        if start < REACH:
            count = min(REACH - start, chunk)
            side = rim_x_ref[start : start + count]
            fix = side[:, :8] + corner_ref[start : start + count]
            edge = jnp.concatenate([edge[:count] + fix, edge[count:]], axis=0)
            rest = jnp.concatenate([part[:count, 8:] + side[:, 8:], part[count:, 8:]], axis=0)
        else:
            rest = part[:, 8:]
        part = jnp.concatenate([edge, rest], axis=1).reshape(chunk * block_y, KZ)
        part_high, part_low = halves(part)
        both = dot(stacked, part_high, NT)
        total = both[:size] + both[size:] + dot(high, part_low, NT)
        out_ref[:, start * block_y : (start + chunk) * block_y] = total


def forward_z(core, rims, high, low):
    import functools

    block_x, block_y = core.shape[:2]
    chunk = 256 // block_y
    return pl.pallas_call(
        functools.partial(forward_z_body, chunk=chunk),
        out_shape=jax.ShapeDtypeStruct((KZ, block_x * block_y), f32),
        in_specs=[vmem] * 6,
        out_specs=vmem,
        name="forward_z",
    )(core, *rims, high, low)


def backward_z_body(in_ref, high_ref, low_ref, core_ref, rim_y_ref, rim_x_ref, corner_ref, energy_ref, *, chunk):
    block_x, block_y = core_ref.shape[:2]
    high = high_ref[...]
    low = low_ref[...]
    for start in range(0, block_x, chunk):
        part = in_ref[:, start * block_y : (start + chunk) * block_y].T
        part_high, part_low = halves(part)
        size = part.shape[0]
        both = dot(jnp.concatenate([part_high, part_low], axis=0), high, NN)
        total = both[:size] + both[size:] + dot(part_high, low, NN)
        total = total.reshape(chunk, block_y, KZ)
        core_ref[start : start + chunk] = total
        rim_y_ref[start : start + chunk] = total[:, :8]
        if start < REACH:
            count = min(REACH - start, chunk)
            rim_x_ref[start : start + count] = total[:count]
            corner_ref[start : start + count] = total[:count, :8]
    tail = in_ref[:, block_x * block_y :]
    energy_ref[...] = jnp.sum(tail.reshape(-1, 8, LANES), axis=0)


def backward_z(spectral, high, low, block_x, block_y):
    import functools

    chunk = 256 // block_y
    shapes = [
        (block_x, block_y, KZ), (block_x, 8, KZ), (REACH, block_y, KZ), (REACH, 8, KZ), (8, LANES),
    ]
    return pl.pallas_call(
        functools.partial(backward_z_body, chunk=chunk),
        out_shape=[jax.ShapeDtypeStruct(s, f32) for s in shapes],
        in_specs=[vmem] * 3,
        out_specs=[vmem] * 5,
        name="backward_z",
    )(spectral, high, low)


def swap_blocks(parts, width):
    lane_at = lax.broadcasted_iota(jnp.int32, parts[0].shape, 1)
    first = lane_at < 2 * width
    even = (lane_at // width) % 2 == 0
    a, b, c, d = parts
    a, c = jnp.where(first, a, pltpu.roll(c, 2 * width, 1)), jnp.where(first, pltpu.roll(a, 2 * width, 1), c)
    b, d = jnp.where(first, b, pltpu.roll(d, 2 * width, 1)), jnp.where(first, pltpu.roll(b, 2 * width, 1), d)
    back = LANES - width
    a, b = jnp.where(even, a, pltpu.roll(b, width, 1)), jnp.where(even, pltpu.roll(a, back, 1), b)
    c, d = jnp.where(even, c, pltpu.roll(d, width, 1)), jnp.where(even, pltpu.roll(c, back, 1), d)
    return [a, b, c, d]


def planes_body(
    where_ref, line_ref, in_ref, y_high_ref, y_low_ref, x_high_ref, x_low_ref, factor_ref, square_ref,
    out_ref, main_ref, twin_ref,
    *, pens, block_x, block_y,
):
    groups = KX // block_x
    high_x = block_x * block_y // LANES
    me = where_ref[0]
    y_high = y_high_ref[...]
    y_low = y_low_ref[...]
    step_rows_count = 256

    def times_y(rows):
        high, low = halves(rows)
        size = rows.shape[0]
        both = dot(jnp.concatenate([high, low], axis=0), y_high, NN)
        total = both[:size] + both[size:] + dot(high, y_low, NN)
        turned = pltpu.roll(total[:, KY:].reshape(size // 8, 8, KY), 4, 1).reshape(size, KY)
        return total[:, :KY], turned

    comp_at = lax.broadcasted_iota(jnp.int32, (step_rows_count, KY), 0) % 8
    sign = jnp.where(comp_at < 4, 1.0, -1.0)
    per_step = step_rows_count // 32

    def forward_step(step, carry):
        group = step // (high_x // per_step)
        first = (step % (high_x // per_step)) * per_step
        rows = []
        for k in range(per_step):
            lanes = pl.ds(pl.multiple_of((first + k) * LANES, LANES), LANES)
            lower = swap_blocks([in_ref[group * pens + p, :, lanes] for p in range(4)], block_y)
            upper = swap_blocks([in_ref[group * pens + 4 + p, :, lanes] for p in range(4)], block_y)
            for low, up in zip(lower, upper):
                rows.append(jnp.concatenate([low, up], axis=1))
        plain, turned = times_y(jnp.concatenate(rows, axis=0))
        at = pl.ds(pl.multiple_of(step * step_rows_count, step_rows_count), step_rows_count)
        main = plain + sign * turned
        twin = sign * plain - turned
        for k in range(2):
            side = slice(k * LANES, (k + 1) * LANES)
            main_ref[k, at, :] = main[:, side]
            twin_ref[k, at, :] = twin[:, side]
        return carry

    lax.fori_loop(0, groups * high_x // per_step, forward_step, 0)

    def times_x(real, imag):
        high, low = halves(jnp.concatenate([real, imag], axis=0))
        x_high = x_high_ref[...]
        total = dot(x_high, high, NN) + dot(x_high, low, NN) + dot(x_low_ref[...], high, NN)
        return total[:KX], total[KX:]

    def plane_of(ref, comp):
        return jnp.concatenate([ref[k, pl.ds(comp, KX, stride=8), :] for k in range(2)], axis=1)

    def influence(entry):
        square = square_ref[...] + line_ref[0, entry]
        value = factor_ref[...] * line_ref[1, entry] / jnp.where(square > 0, square, 1.0)
        return jnp.where(square > 0, value, 0.0)

    energy = jnp.zeros((KX, KY), f32)
    for plane in range(4):
        real, imag = times_x(plane_of(main_ref, plane), plane_of(main_ref, plane + 4))
        kernel = influence(me * 4 + plane)
        if plane == 0:
            mine = me == 0
            other = influence(KZ // 2)
            share = jnp.where(mine, 0.5 * (kernel + other), kernel)
            cross = jnp.where(mine, 0.5 * (kernel - other), 0.0)
            twin_real, twin_imag = times_x(plane_of(twin_ref, 0), plane_of(twin_ref, 4))
            out_real = share * real + cross * twin_real
            out_imag = share * imag + cross * twin_imag
            energy = energy + jnp.where(mine, 0.5, 1.0) * (real * out_real + imag * out_imag)
        else:
            out_real = kernel * real
            out_imag = kernel * imag
            energy = energy + (real * out_real + imag * out_imag)
        real, imag = times_x(out_real, -out_imag)
        for k in range(2):
            side = slice(k * LANES, (k + 1) * LANES)
            main_ref[k, pl.ds(plane, KX, stride=8), :] = real[:, side]
            main_ref[k, pl.ds(plane + 4, KX, stride=8), :] = -imag[:, side]

    total = jnp.sum(jnp.sum(energy, axis=0, keepdims=True), axis=1, keepdims=True)
    out_ref[:, :, block_x * block_y :] = jnp.broadcast_to(
        total.reshape(1, 1, 1), (groups * pens, 8, LANES)
    )

    def backward_step(step, carry):
        group = step // (high_x // per_step)
        first = (step % (high_x // per_step)) * per_step
        at = pl.ds(pl.multiple_of(step * step_rows_count, step_rows_count), step_rows_count)
        plain, turned = times_y(jnp.concatenate([main_ref[0, at, :], main_ref[1, at, :]], axis=1))
        rows = plain - sign * turned
        for k in range(per_step):
            lanes = pl.ds(pl.multiple_of((first + k) * LANES, LANES), LANES)
            pieces = [rows[(4 * k + j) * 8 : (4 * k + j + 1) * 8] for j in range(4)]
            lower = swap_blocks([piece[:, :LANES] for piece in pieces], block_y)
            upper = swap_blocks([piece[:, LANES:] for piece in pieces], block_y)
            for p in range(4):
                out_ref[group * pens + p, :, lanes] = lower[p]
                out_ref[group * pens + 4 + p, :, lanes] = upper[p]
        return carry

    lax.fori_loop(0, groups * high_x // per_step, backward_step, 0)


def solve_planes(incoming, me, pens, block_x, block_y):
    import functools

    angle = angles(np.arange(KY), np.arange(KY), KY)
    y_high, y_low = table_halves(np.concatenate([np.cos(angle), np.sin(angle)], axis=1))
    angle = angles(np.arange(KX), np.arange(KX), KX)
    cos_x, sin_x = np.cos(angle), np.sin(angle)
    x_high, x_low = table_halves(np.block([[cos_x, sin_x], [-sin_x, cos_x]]))
    square_x, factor_x = np_line(KX)
    square_y, factor_y = np_line(KY)
    square_z, factor_z = np_line(KZ)
    factor = jnp.asarray(np.float32(np.outer(factor_x, factor_y) / (math.pi * KX * KY * KZ)))
    square = jnp.asarray(np.float32(square_x[:, None] + square_y[None, :]))
    line = jnp.asarray(np.float32(np.stack([square_z, factor_z])))
    devices, comps, lanes = incoming.shape
    body = functools.partial(planes_body, pens=pens, block_x=block_x, block_y=block_y)
    return pl.pallas_call(
        body,
        out_shape=jax.ShapeDtypeStruct((devices, comps, lanes + LANES), f32),
        in_specs=[smem, smem] + [vmem] * 7,
        out_specs=vmem,
        scratch_shapes=[pltpu.VMEM((2, KX * 8, LANES), f32)] * 2,
        name="planes",
    )(me.reshape(1), line, incoming, y_high, y_low, x_high, x_low, factor, square)


def modulus(index, length):
    coeffs = (1.0 / 120.0, 26.0 / 120.0, 66.0 / 120.0, 26.0 / 120.0, 1.0 / 120.0)
    real_part = 0.0
    imag_part = 0.0
    for j in range(5):
        angle = (index * j % length).astype(jnp.float32) * (2.0 * math.pi / length)
        real_part = real_part + coeffs[j] * jnp.cos(angle)
        imag_part = imag_part + coeffs[j] * jnp.sin(angle)
    return real_part * real_part + imag_part * imag_part


def influence(index_x, index_y, index_z):
    freq_x = jnp.where(2 * index_x < KX, index_x, index_x - KX).astype(jnp.float32) / KX
    freq_y = jnp.where(2 * index_y < KY, index_y, index_y - KY).astype(jnp.float32) / KY
    freq_z = jnp.where(2 * index_z < KZ, index_z, index_z - KZ).astype(jnp.float32) / KZ
    square = freq_x * freq_x + freq_y * freq_y + freq_z * freq_z
    safe = jnp.where(square > 0, square, 1.0)
    volume = float(KX * KY * KZ)
    value = jnp.exp(-math.pi**2 * safe / ewald_split**2) / (math.pi * volume * safe)
    value = value / (modulus(index_x, KX) * modulus(index_y, KY) * modulus(index_z, KZ))
    return jnp.where(square > 0, value, 0.0)


def dft_tables(length):
    index = jnp.arange(length, dtype=jnp.int32)
    angle = (index[:, None] * index[None, :] % length).astype(jnp.float32) * (
        2.0 * math.pi / length
    )
    return (jnp.cos(angle), jnp.sin(angle))


def z_slots(groups):
    planes = KZ // (2 * groups) + 1
    owner = jnp.arange(groups, dtype=jnp.int32)[:, None]
    within = jnp.arange(planes, dtype=jnp.int32)[None, :]
    ordinary = owner * (planes - 1) + within
    frequency = jnp.where(within < planes - 1, ordinary, jnp.where(owner == 0, KZ // 2, 0))
    plane_weight = jnp.where(
        within < planes - 1, jnp.where(frequency == 0, 1.0, 2.0), jnp.where(owner == 0, 1.0, 0.0)
    )
    frequency = frequency.reshape(-1)
    plane_weight = plane_weight.reshape(-1).astype(jnp.float32)
    position = jnp.arange(KZ, dtype=jnp.int32)
    angle = (frequency[:, None] * position[None, :] % KZ).astype(jnp.float32) * (2.0 * math.pi / KZ)
    usable = (plane_weight > 0).astype(jnp.float32)[:, None]
    return (planes, frequency, plane_weight, jnp.cos(angle) * usable, jnp.sin(angle) * usable)


def forward_complex(data, cos_table, sin_table, shape, axis):
    direct = jnp.dot(cos_table, data, precision=highest).reshape(shape)
    other = jnp.dot(sin_table, data, precision=highest).reshape(shape)
    real_part = jnp.take(direct, 0, axis=axis) + jnp.take(other, 1, axis=axis)
    imag_part = jnp.take(direct, 1, axis=axis) - jnp.take(other, 0, axis=axis)
    return (real_part, imag_part)


def inverse_complex(data, cos_table, sin_table, shape, axis):
    direct = jnp.dot(cos_table, data, precision=highest).reshape(shape)
    other = jnp.dot(sin_table, data, precision=highest).reshape(shape)
    real_part = jnp.take(direct, 0, axis=axis) - jnp.take(other, 1, axis=axis)
    imag_part = jnp.take(other, 0, axis=axis) + jnp.take(direct, 1, axis=axis)
    return (real_part, imag_part)


def spectrum_pen_first(grid, block_x, block_y):
    cos_x, sin_x = dft_tables(KX)
    cos_y, sin_y = dft_tables(KY)
    planes, frequency, plane_weight, cos_z, sin_z = z_slots(lax.axis_size("pen"))
    slot_total = cos_z.shape[0]
    lines = KY // lax.axis_size("grp")
    real_z = jnp.einsum("xyz,kz->ykx", grid, cos_z, precision=highest)
    imag_z = -jnp.einsum("xyz,kz->ykx", grid, sin_z, precision=highest)
    outgoing = jnp.stack([real_z, imag_z], axis=2).reshape(block_y, slot_total * 2 * block_x)
    columns = lax.all_to_all(outgoing, "pen", split_axis=1, concat_axis=0, tiled=True)
    real_y, imag_y = forward_complex(columns, cos_y, sin_y, (KY, planes, 2, block_x), 2)
    sectioned = jnp.transpose(jnp.stack([real_y, imag_y], axis=-1), (2, 0, 1, 3)).reshape(
        block_x, KY * planes * 2
    )
    rows = lax.all_to_all(sectioned, "grp", split_axis=1, concat_axis=0, tiled=True)
    real_x, imag_x = forward_complex(rows, cos_x, sin_x, (KX, lines, planes, 2), 3)
    first = lax.axis_index("pen") * planes
    index_x = jnp.arange(KX, dtype=jnp.int32)[:, None, None]
    index_y = lax.axis_index("grp") * lines + jnp.arange(lines, dtype=jnp.int32)[None, :, None]
    index_z = lax.dynamic_slice_in_dim(frequency, first, planes)[None, None, :]
    local_weight = lax.dynamic_slice_in_dim(plane_weight, first, planes)[None, None, :]
    kernel = influence(index_x, index_y, index_z)
    spectral = 0.5 * jnp.sum(local_weight * kernel * (real_x * real_x + imag_x * imag_x))
    scaled = jnp.stack([kernel * real_x, kernel * imag_x], axis=-1).reshape(KX, lines * planes * 2)
    real_b, imag_b = inverse_complex(scaled, cos_x, sin_x, (KX, lines, planes, 2), 3)
    returning = jnp.stack([real_b, imag_b], axis=-1).reshape(KX, lines * planes * 2)
    rows_home = lax.all_to_all(returning, "grp", split_axis=0, concat_axis=1, tiled=True)
    rows_home = jnp.transpose(rows_home.reshape(block_x, KY, planes, 2), (1, 2, 3, 0)).reshape(
        KY, planes * 2 * block_x
    )
    real_c, imag_c = inverse_complex(rows_home, cos_y, sin_y, (KY, planes, 2, block_x), 2)
    leaving = jnp.stack([real_c, imag_c], axis=2).reshape(KY, planes * 2 * block_x)
    home = lax.all_to_all(leaving, "pen", split_axis=0, concat_axis=1, tiled=True).reshape(
        block_y, slot_total, 2, block_x
    )
    potential = jnp.einsum(
        "ykx,kz->xyz", home[:, :, 0], plane_weight[:, None] * cos_z, precision=highest
    )
    potential = potential - jnp.einsum(
        "ykx,kz->xyz", home[:, :, 1], plane_weight[:, None] * sin_z, precision=highest
    )
    return (potential, spectral)


def local(cell_offsets, cell_z, frac, charges, tile_counts):
    groups_all, pens = lax.axis_size("grp"), lax.axis_size("pen")
    devices = groups_all * pens
    block_x = KX // groups_all
    block_y = KY // pens
    tiles = tile_counts.shape[0]
    slots = charges.shape[0] // tiles
    tiles_y = block_y // 2
    groups = tiles_y * slots // (2 * LANES)
    lines = charges.shape[0] // LANES
    offs = cell_offsets.reshape(2, lines, LANES)
    fracs = frac.reshape(3, lines, LANES)
    zcell = cell_z.reshape(lines, LANES)
    charge = charges.reshape(lines, LANES)
    sizes = (slots, groups, block_x, block_y)
    core, rim_y, rim_x, corner = spread_charges(tile_counts, fracs, offs, zcell, charge, *sizes)
    rims = (shifted(rim_y, "pen", 1), shifted(rim_x, "grp", 1), shifted_both(corner, 1))
    by_planes = KZ == 8 * devices and 4 * block_y == LANES and pens == 8
    if by_planes:
        forward, back = z_table(devices)
        spectral = forward_z(core, rims, *table_halves(forward)).reshape(devices, 8, block_x * block_y)
        spectral = lax.all_to_all(spectral, ("grp", "pen"), 0, 0, tiled=True)
        spectral = solve_planes(spectral, lax.axis_index(("grp", "pen")), pens, block_x, block_y)
        spectral = lax.all_to_all(spectral, ("grp", "pen"), 0, 0, tiled=True)
        core, rim_y, rim_x, corner, parts = backward_z(
            spectral.reshape(KZ, -1), *table_halves(back.reshape(KZ, KZ)), block_x, block_y
        )
        total = parts[0, 0]
    else:
        grid = core.at[:, :8].add(rims[0]).at[:REACH].add(rims[1]).at[:REACH, :8].add(rims[2])
        core, share = spectrum_pen_first(grid, block_x, block_y)
        rim_y, rim_x, corner = core[:, :8], core[:REACH], core[:REACH, :8]
        total = lax.psum(share, ("grp", "pen"))
    rims = (shifted(rim_y, "pen", -1), shifted(rim_x, "grp", -1), shifted_both(corner, -1))
    forces = interpolate(tile_counts, fracs, offs, zcell, charge, core, rims, *sizes)
    return (forces.reshape(3, lines * LANES), total / (charges.shape[0] * devices))


def solution(mesh):
    in_specs = (
        P(None, ("grp", "pen")),
        P(("grp", "pen")),
        P(None, ("grp", "pen")),
        P(("grp", "pen")),
        P(("grp", "pen")),
    )
    out_specs = (P(None, ("grp", "pen")), P())
    return jax.shard_map(local, mesh=mesh, in_specs=in_specs, out_specs=out_specs, check_vma=False)
```

```python
import functools
import math

import jax
import jax.numpy as jnp
import numpy as np
from jax import lax
from jax.experimental import pallas as pl
from jax.experimental.pallas import tpu as pltpu
from jax.sharding import PartitionSpec as P

KX = 256
KY = 256
KZ = 256
LANES = 128
ROWS = 16
SPAN = 7
REACH = 5

ewald_split = 0.6
highest = lax.Precision.HIGHEST
f32 = jnp.float32
bf16 = jnp.bfloat16


def shifted(block, axis, distance):
    devices = range(lax.axis_size(axis))
    route = [((i - distance) % len(devices), i) for i in devices]
    return lax.ppermute(block, axis, route)


def shifted_both(block, distance):
    groups, pens = lax.axis_size("grp"), lax.axis_size("pen")
    route = []
    for g in range(groups):
        for p in range(pens):
            source = ((g - distance) % groups) * pens + (p - distance) % pens
            route.append((source, g * pens + p))
    return lax.ppermute(block, ("grp", "pen"), route)


def halves(value):
    high = value.astype(bf16)
    low = (value - high.astype(f32)).astype(bf16)
    return high, low


def table_halves(table):
    table = jnp.asarray(np.asarray(table, np.float32))
    return halves(table)


def dot(left, right, dims):
    return lax.dot_general(left, right, (dims, ((), ())), preferred_element_type=f32)


NN = ((1,), (0,))
NT = ((1,), (1,))


def spline_rows(x):
    values = [jnp.ones_like(x)]
    fifth = None
    for order in range(2, 7):
        nxt = []
        for j in range(order):
            term = None
            if j >= 1:
                term = values[j - 1] * (x + float(order - 1 - j))
            if j <= order - 2:
                other = values[j] * (float(1 + j) - x)
                term = other if term is None else term + other
            nxt.append(term)
        if order == 5:
            fifth = [v * (1.0 / 24.0) for v in nxt]
        values = nxt
    thetas = [v * (1.0 / 120.0) for v in values]
    slopes = [-fifth[0]]
    for j in range(1, 5):
        slopes.append(fifth[j - 1] - fifth[j])
    slopes.append(fifth[4])
    return thetas, slopes


def placed(rows, offset):
    out = []
    zero = jnp.zeros_like(rows[0])
    for i in range(SPAN):
        here = rows[i] if i <= 5 else zero
        before = rows[i - 1] if i >= 1 else zero
        out.append(jnp.where(offset == 0, here, before))
    return out


def spread_out(row):
    return jnp.broadcast_to(row, (ROWS, row.shape[-1]))


def group_places(step, ranges):
    places = []
    for k in range(4):
        index = step * 4 + k
        passed = 0
        row = col = 0
        for first, last, low, high in ranges:
            width = high - low
            inside = index - passed
            a, g = first + inside // width, low + inside % width
            row, col = (a, g) if passed == 0 else (jnp.where(inside >= 0, a, row), jnp.where(inside >= 0, g, col))
            passed += (last - first) * width
        places.append((row, col))
    return places


def step_count(ranges):
    return sum((last - first) * (high - low) for first, last, low, high in ranges) // 4


def step_atoms(places, refs, slots, groups):
    counts_ref, frac_ref, offs_ref, z_ref, q_ref = refs
    per_row = LANES // slots
    lines = [(a * groups + g) * 2 + half for a, g in places for half in range(2)]

    def wide(ref, d):
        rows = [ref[d : d + 1, pl.ds(pl.multiple_of(line * LANES, LANES), LANES)] for line in lines]
        return jnp.concatenate(rows, axis=0)

    def tall(ref):
        return jnp.concatenate([ref[pl.ds(line, 1), :] for line in lines], axis=0)

    row_at = lax.broadcasted_iota(jnp.int32, (8, LANES), 0)
    lane_at = lax.broadcasted_iota(jnp.int32, (8, LANES), 1)
    tile_at = row_at * per_row + lane_at // slots
    count = jnp.zeros((8, LANES), jnp.int32)
    for r, line in enumerate(lines):
        for k in range(per_row):
            count = jnp.where(tile_at == r * per_row + k, counts_ref[line * per_row + k], count)
    charge = jnp.where(lane_at % slots < count, tall(q_ref), 0.0)
    tile_in_group = (row_at % 2) * per_row + lane_at // slots
    fracs = [wide(frac_ref, d) for d in range(3)]
    return fracs, wide(offs_ref, 0), wide(offs_ref, 1) + 2 * tile_in_group, tall(z_ref), charge, lines


def keep_rows(tab_ref, lists):
    for q, rows in enumerate(lists):
        for j, value in enumerate(rows):
            tab_ref[pl.ds(64 * q + 8 * j, 8), :] = value


def clear_rows(tab_ref):
    tab_ref[...] = jnp.zeros_like(tab_ref)


def by_distance(distance, tab_ref, q, row):
    table = tab_ref[pl.ds(64 * q + row, 8, stride=8), :]
    at = jnp.minimum(distance & 15, 7)
    return jnp.concatenate(
        [jnp.take_along_axis(table, at[k : k + 8], axis=0, mode="promise_in_bounds") for k in (0, 8)], axis=0
    )


def z_parts(zcell, row, tab_ref, lists):
    cell = spread_out(zcell[row : row + 1])
    at = lax.broadcasted_iota(jnp.int32, (ROWS, LANES), 0)
    ahead = (at - cell) & (ROWS - 1)
    block = ((cell + ahead) & (KZ - 1)) // ROWS
    weights = [by_distance(ahead, tab_ref, q, row) for q in lists]
    return block.astype(f32).astype(bf16), weights


def z_matrix(block, weight):
    zero = jnp.zeros_like(weight)
    return jnp.concatenate(
        [jnp.where(block == jnp.array(k, bf16), weight, zero) for k in range(KZ // ROWS)], axis=0
    )


def spread_body(*refs, slots, groups, ranges, base, pieces, carried):
    atom_refs = refs[:5]
    acc_ref, tab_ref = refs[-2:]
    acc_ref[...] = jnp.zeros_like(acc_ref)
    clear_rows(tab_ref)
    for piece, ref in zip(carried, refs[5:]):
        low = (piece[0] - base, piece[2])
        acc_ref[low[0] : low[0] + ref.shape[0], low[1] : low[1] + ref.shape[1]] += ref[...]
    refs = refs[5 + len(carried) :]
    at = lax.broadcasted_iota(jnp.int32, (ROWS, LANES), 0)

    def body(step, carry):
        places = group_places(step, ranges)
        fracs, offset_x, offset_y, zcell, charge, lines = step_atoms(places, atom_refs, slots, groups)
        theta_x, _ = spline_rows(fracs[0])
        theta_y, _ = spline_rows(fracs[1])
        theta_z, _ = spline_rows(fracs[2])
        theta_y = [t * charge for t in theta_y]
        weight_x = placed(theta_x, offset_x)
        keep_rows(tab_ref, [theta_z, theta_y])
        for k in range(4):
            blocks, zs, pairs = [], [], []
            for half in range(2):
                line = 2 * k + half
                row = slice(line, line + 1)
                block, (weight,) = z_parts(zcell, line, tab_ref, [0])
                blocks.append(block)
                zs.append(weight)
                weight_y = by_distance(at - spread_out(offset_y[row]), tab_ref, 1, line)
                pairs.append([spread_out(weight_x[i][row]) * weight_y for i in range(SPAN)])
            block = jnp.concatenate(blocks, axis=1)
            z_high, z_low = halves(jnp.concatenate(zs, axis=1))
            table_high = z_matrix(block, z_high)
            table_low = z_matrix(block, z_low)
            pair = jnp.concatenate(
                [jnp.concatenate([pairs[0][i], pairs[1][i]], axis=1) for i in range(SPAN)], axis=0
            )
            high, low = halves(pair)
            both = dot(jnp.concatenate([high, low], axis=0), table_high, NT)
            rest = dot(high, table_low, NT)
            total = both[: SPAN * ROWS] + both[SPAN * ROWS :] + rest
            a, g = places[k]
            where = (pl.ds(2 * a - base, SPAN), pl.ds(pl.multiple_of(8 * g, 8), ROWS))
            acc_ref[where[0], where[1], :] += total.reshape(SPAN, ROWS, KZ)
        return carry

    lax.fori_loop(0, step_count(ranges), body, 0)
    for piece, ref in zip(pieces, refs):
        ref[...] = acc_ref[piece[0] - base : piece[1] - base, piece[2] : piece[3], :]


vmem = pl.BlockSpec(memory_space=pltpu.VMEM)
room = pltpu.CompilerParams(vmem_limit_bytes=28 * 1024 * 1024)


def resident(values):
    return [pltpu.with_memory_space_constraint(value, pltpu.VMEM) for value in values]


def apart(values):
    return [pltpu.with_memory_space_constraint(value, pltpu.HBM) for value in values]


def kept(shape):
    return pltpu.VMEM(shape, f32)


def stored(shape):
    return pltpu.HBM(shape, f32)


smem = pl.BlockSpec(memory_space=pltpu.SMEM)


def spread_charges(atoms, slots, groups, block_y, ranges, pieces, holds, carried=(), fields=()):
    base = min([2 * r[0] for r in ranges] + [p[0] for p in pieces + list(carried)])
    top = max([2 * r[1] + REACH for r in ranges] + [p[1] for p in pieces + list(carried)])
    body = functools.partial(
        spread_body, slots=slots, groups=groups, ranges=ranges, base=base, pieces=pieces, carried=carried
    )
    shapes = [(p[1] - p[0], p[3] - p[2], KZ) for p in pieces]
    return pl.pallas_call(
        body,
        out_shape=[hold(s) for hold, s in zip(holds, shapes)],
        in_specs=[smem] + [vmem] * (4 + len(fields)),
        compiler_params=room,
        out_specs=[vmem] * len(shapes),
        scratch_shapes=[pltpu.VMEM((top - base, block_y + 8, KZ), f32), pltpu.VMEM((128, LANES), f32)],
        name="spread",
    )(*atoms, *fields)


def interp_body(*refs, slots, groups, ranges, base, pieces, before, first):
    atom_refs = refs[:5]
    out_ref, pot_ref, tab_ref = refs[-3:]
    clear_rows(tab_ref)
    refs = refs[5:]
    for (low_x, low_y, skip), ref in zip(pieces, refs):
        tall, wide = ref.shape[0] - skip, ref.shape[1]
        pot_ref[low_x + skip - base : low_x + skip - base + tall, low_y : low_y + wide, :] = ref[skip:]
    for k in range(before):
        earlier_ref = refs[len(pieces) + k]
        start = earlier_ref.shape[1] * k if k == 0 else out_ref.shape[1] - earlier_ref.shape[1]
        out_ref[:, start : start + earlier_ref.shape[1]] = earlier_ref[...]
    at = lax.broadcasted_iota(jnp.int32, (ROWS, LANES), 0)
    height = SPAN * ROWS

    def body(step, carry):
        places = group_places(step, ranges)
        fracs, offset_x, offset_y, zcell, charge, lines = step_atoms(places, atom_refs, slots, groups)
        theta_x, slope_x = spline_rows(fracs[0])
        theta_y, slope_y = spline_rows(fracs[1])
        theta_z, slope_z = spline_rows(fracs[2])
        theta_y = [t * -charge for t in theta_y]
        slope_y = [t * -charge for t in slope_y]
        weight_x = placed(theta_x, offset_x)
        grade_x = placed(slope_x, offset_x)
        keep_rows(tab_ref, [theta_z, slope_z, theta_y, slope_y])
        for k in range(4):
            blocks, zs, gs = [], [], []
            for half in range(2):
                block, (weight, grade) = z_parts(zcell, 2 * k + half, tab_ref, [0, 1])
                blocks.append(block)
                zs.append(weight)
                gs.append(grade)
            block = jnp.concatenate(blocks, axis=1)
            z_high, z_low = halves(jnp.concatenate(zs, axis=1))
            g_high, g_low = halves(jnp.concatenate(gs, axis=1))
            a, g = places[k]
            slab = pot_ref[pl.ds(2 * a - base, SPAN), pl.ds(pl.multiple_of(8 * g, 8), ROWS), :]
            high, low = halves(slab.reshape(height, KZ))
            stacked = jnp.concatenate([high, low], axis=0)
            main = dot(stacked, z_matrix(block, z_high), NN)
            main = main[:height] + main[height:] + dot(high, z_matrix(block, z_low), NN)
            tilt = dot(stacked, z_matrix(block, g_high), NN)
            tilt = tilt[:height] + tilt[height:] + dot(high, z_matrix(block, g_low), NN)
            for half in range(2):
                row = slice(2 * k + half, 2 * k + half + 1)
                lanes = slice(half * LANES, (half + 1) * LANES)
                away = at - spread_out(offset_y[row])
                weight_y = by_distance(away, tab_ref, 2, 2 * k + half)
                grade_y = by_distance(away, tab_ref, 3, 2 * k + half)
                plain = steep = tilted = 0.0
                for i in range(SPAN):
                    part = slice(i * ROWS, (i + 1) * ROWS)
                    wide = spread_out(weight_x[i][row])
                    plain = plain + wide * main[part, lanes]
                    tilted = tilted + wide * tilt[part, lanes]
                    steep = steep + spread_out(grade_x[i][row]) * main[part, lanes]
                forces = [
                    jnp.sum(steep * weight_y, axis=0, keepdims=True),
                    jnp.sum(plain * grade_y, axis=0, keepdims=True),
                    jnp.sum(tilted * weight_y, axis=0, keepdims=True),
                ]
                start = (lines[2 * k + half] - first) * LANES
                out_ref[:, pl.ds(pl.multiple_of(start, LANES), LANES)] = jnp.concatenate(forces, axis=0)
        return carry

    lax.fori_loop(0, step_count(ranges), body, 0)


def interpolate(atoms, slots, groups, block_y, ranges, pieces, fields, rows, hold, earlier=()):
    base = min(2 * r[0] for r in ranges)
    line = 2 * groups
    body = functools.partial(
        interp_body, slots=slots, groups=groups, ranges=ranges, base=base, pieces=pieces,
        before=len(earlier), first=rows[0] * line,
    )
    height = max(max(2 * r[1] + REACH for r in ranges), max(p[0] + f.shape[0] for p, f in zip(pieces, fields))) - base
    return pl.pallas_call(
        body,
        out_shape=hold((3, (rows[1] - rows[0]) * line * LANES)),
        in_specs=[smem] + [vmem] * (4 + len(fields) + len(earlier)),
        compiler_params=room,
        out_specs=vmem,
        scratch_shapes=[pltpu.VMEM((height, block_y + 8, KZ), f32), pltpu.VMEM((256, LANES), f32)],
        name="interpolate",
    )(*atoms, *fields, *earlier)


def angles(left, right, length):
    return (np.outer(left, right) % length) * (2.0 * math.pi / length)


def np_modulus(length):
    index = np.arange(length)
    coeffs = (1.0 / 120.0, 26.0 / 120.0, 66.0 / 120.0, 26.0 / 120.0, 1.0 / 120.0)
    total = 0.0
    for j in range(5):
        total = total + coeffs[j] * np.exp(2j * math.pi * ((index * j) % length) / length)
    return np.abs(total) ** 2


def np_line(length):
    index = np.arange(length)
    freq = np.where(2 * index < length, index, index - length) / length
    square = freq * freq
    return square, np.exp(-(math.pi**2) * square / ewald_split**2) / np_modulus(length)


def z_table(devices):
    per = KZ // 2 // devices
    position = np.arange(KZ)
    forward, back = [], []
    for device in range(devices):
        for imaginary in range(2):
            for plane in range(device * per, (device + 1) * per):
                wave = 2.0 * math.pi * ((plane * position) % KZ) / KZ
                if plane == 0:
                    row = np.where(position % 2 == 0, 1.0, -1.0) if imaginary else np.ones(KZ)
                    forward.append(row)
                    back.append(row)
                else:
                    row = -np.sin(wave) if imaginary else np.cos(wave)
                    forward.append(row)
                    back.append(2.0 * row)
    return np.stack(forward), np.stack(back)


def forward_z_body(core_ref, rim_y_ref, *refs, chunk, first):
    out_ref = refs[-1]
    high = refs[-3][...]
    low = refs[-2][...]
    sides = refs[:-3]
    block_x, block_y = core_ref.shape[:2]
    stacked = jnp.concatenate([high, low], axis=0)
    size = high.shape[0]
    for start in range(0, block_x, chunk):
        part = core_ref[start : start + chunk]
        edge = part[:, :8] + rim_y_ref[first + start : first + start + chunk]
        rest = part[:, 8:]
        if sides and start < REACH:
            count = min(REACH - start, chunk)
            side = sides[0][start : start + count]
            fix = side[:, :8] + sides[1][start : start + count]
            edge = jnp.concatenate([edge[:count] + fix, edge[count:]], axis=0)
            rest = jnp.concatenate([rest[:count] + side[:, 8:], rest[count:]], axis=0)
        part = jnp.concatenate([edge, rest], axis=1).reshape(chunk * block_y, KZ)
        part_high, part_low = halves(part)
        both = dot(stacked, part_high, NT)
        total = both[:size] + both[size:] + dot(high, part_low, NT)
        out_ref[:, start * block_y : (start + chunk) * block_y] = total


def forward_z(core, rims, high, low, first):
    block_x, block_y = core.shape[:2]
    chunk = 256 // block_y
    return pl.pallas_call(
        functools.partial(forward_z_body, chunk=chunk, first=first),
        out_shape=kept((KZ, block_x * block_y)),
        in_specs=[vmem] * (3 + len(rims)),
        compiler_params=room,
        out_specs=vmem,
        name="forward_z",
    )(*resident([core, *rims]), high, low)


def backward_z_body(in_ref, high_ref, low_ref, core_ref, rim_y_ref, *refs, chunk, scale):
    block_x, block_y = core_ref.shape[:2]
    high = high_ref[...]
    low = low_ref[...]
    for start in range(0, block_x, chunk):
        part = in_ref[:, start * block_y : (start + chunk) * block_y].T
        part_high, part_low = halves(part)
        size = part.shape[0]
        both = dot(jnp.concatenate([part_high, part_low], axis=0), high, NN)
        total = both[:size] + both[size:] + dot(part_high, low, NN)
        total = total.reshape(chunk, block_y, KZ)
        core_ref[start : start + chunk] = total
        rim_y_ref[start : start + chunk] = total[:, :8]
        if len(refs) == 3:
            if start < REACH:
                count = min(REACH - start, chunk)
                refs[0][start : start + count] = total[:count]
                refs[1][start : start + count] = total[:count, :8]
            over = block_x - refs[2].shape[0]
            if start >= over:
                refs[2][start - over : start - over + chunk] = total
    if len(refs) == 1:
        tail = in_ref[:, block_x * block_y :]
        refs[0][0] = jnp.max(jnp.sum(tail.reshape(-1, 8, LANES), axis=0)) * scale


def backward_z(spectral, high, low, block_x, block_y, others, scale=None):
    chunk = 256 // block_y
    sent = [(block_x, 8, KZ)] + others
    total = [] if scale is None else [jax.ShapeDtypeStruct((1,), f32)]
    return pl.pallas_call(
        functools.partial(backward_z_body, chunk=chunk, scale=scale),
        out_shape=[kept((block_x, block_y, KZ))] + [stored(s) for s in sent] + total,
        in_specs=[vmem] * 3,
        compiler_params=room,
        out_specs=[vmem] * (1 + len(sent)) + [smem] * len(total),
        name="backward_z",
    )(*resident([spectral]), *apart([high, low]))


def swap_blocks(parts, width):
    lane_at = lax.broadcasted_iota(jnp.int32, parts[0].shape, 1)
    first = lane_at < 2 * width
    even = (lane_at // width) % 2 == 0
    a, b, c, d = parts
    a, c = jnp.where(first, a, pltpu.roll(c, 2 * width, 1)), jnp.where(first, pltpu.roll(a, 2 * width, 1), c)
    b, d = jnp.where(first, b, pltpu.roll(d, 2 * width, 1)), jnp.where(first, pltpu.roll(b, 2 * width, 1), d)
    back = LANES - width
    a, b = jnp.where(even, a, pltpu.roll(b, width, 1)), jnp.where(even, pltpu.roll(a, back, 1), b)
    c, d = jnp.where(even, c, pltpu.roll(d, width, 1)), jnp.where(even, pltpu.roll(c, back, 1), d)
    return [a, b, c, d]


STEP = 256


def times_y(rows, y_high, y_low):
    high, low = halves(rows)
    size = rows.shape[0]
    both = dot(jnp.concatenate([high, low], axis=0), y_high, NN)
    total = both[:size] + both[size:] + dot(high, y_low, NN)
    turned = pltpu.roll(total[:, KY:].reshape(size // 8, 8, KY), 4, 1).reshape(size, KY)
    return total[:, :KY], turned


def row_sign():
    comp_at = lax.broadcasted_iota(jnp.int32, (STEP, KY), 0) % 8
    return jnp.where(comp_at < 4, 1.0, -1.0)


def forward_y(in_ref, y_high_ref, y_low_ref, main_ref, twin_ref, pens, width):
    y_high = y_high_ref[...]
    y_low = y_low_ref[...]
    sign = row_sign()
    per_step = STEP // 32
    spans = in_ref.shape[2] // LANES // per_step
    groups = in_ref.shape[0] // pens

    def body(step, carry):
        group = step // spans
        rows = []
        for k in range(per_step):
            at = (step % spans) * per_step + k
            lanes = pl.ds(pl.multiple_of(at * LANES, LANES), LANES)
            lower = swap_blocks([in_ref[group * pens + p, :, lanes] for p in range(4)], width)
            upper = swap_blocks([in_ref[group * pens + 4 + p, :, lanes] for p in range(4)], width)
            for low, up in zip(lower, upper):
                rows.append(jnp.concatenate([low, up], axis=1))
        plain, turned = times_y(jnp.concatenate(rows, axis=0), y_high, y_low)
        at = pl.ds(pl.multiple_of(step * STEP, STEP), STEP)
        main = plain + sign * turned
        twin = sign * plain - turned
        for k in range(2):
            side = slice(k * LANES, (k + 1) * LANES)
            main_ref[k, at, :] = main[:, side]
            twin_ref[k, at, :] = twin[:, side]
        return carry

    lax.fori_loop(0, groups * spans, body, 0)


def backward_y(main_ref, y_high_ref, y_low_ref, out_ref, pens, width, lines):
    y_high = y_high_ref[...]
    y_low = y_low_ref[...]
    sign = row_sign()
    per_step = STEP // 32
    spans = lines // LANES // per_step
    groups = out_ref.shape[0] // pens

    def body(step, carry):
        group = step // spans
        at = pl.ds(pl.multiple_of(step * STEP, STEP), STEP)
        joined = jnp.concatenate([main_ref[0, at, :], main_ref[1, at, :]], axis=1)
        plain, turned = times_y(joined, y_high, y_low)
        rows = plain - sign * turned
        for k in range(per_step):
            at = (step % spans) * per_step + k
            lanes = pl.ds(pl.multiple_of(at * LANES, LANES), LANES)
            pieces = [rows[(4 * k + j) * 8 : (4 * k + j + 1) * 8] for j in range(4)]
            lower = swap_blocks([piece[:, :LANES] for piece in pieces], width)
            upper = swap_blocks([piece[:, LANES:] for piece in pieces], width)
            for p in range(4):
                out_ref[group * pens + p, :, lanes] = lower[p]
                out_ref[group * pens + 4 + p, :, lanes] = upper[p]
        return carry

    lax.fori_loop(0, groups * spans, body, 0)


def planes_first_body(in_ref, y_high_ref, y_low_ref, main_ref, twin_ref, *, pens, width):
    forward_y(in_ref, y_high_ref, y_low_ref, main_ref, twin_ref, pens, width)


def planes_last_body(main_ref, energy_ref, y_high_ref, y_low_ref, out_ref, *, pens, width, lines):
    backward_y(main_ref, y_high_ref, y_low_ref, out_ref, pens, width, lines)
    out_ref[:, :, lines:] = jnp.broadcast_to(energy_ref[...].reshape(1, 8, LANES), (out_ref.shape[0], 8, LANES))


def planes_body(
    where_ref, line_ref, in_ref, far_ref, far_twin_ref, y_high_ref, y_low_ref, x_high_ref, x_low_ref,
    column_ref, row_ref, out_ref, far_out_ref, energy_ref, main_ref, twin_ref,
    *, pens, width,
):
    me = where_ref[0]
    forward_y(in_ref, y_high_ref, y_low_ref, main_ref, twin_ref, pens, width)
    near = main_ref.shape[1] // 8

    def times_x(real, imag):
        high, low = [
            jnp.concatenate(
                [jnp.concatenate([r, i], axis=1), jnp.concatenate([i, -r], axis=1)], axis=0
            )
            for r, i in zip(halves(real), halves(imag))
        ]
        x_high = x_high_ref[...]
        total = dot(x_high, high, NN) + dot(x_high, low, NN) + dot(x_low_ref[...], high, NN)
        return total[:, :KY], total[:, KY:]

    def plane_of(near_ref, far_ref, comp):
        def whole(ref):
            return jnp.concatenate([ref[k, pl.ds(comp, ref.shape[1] // 8, stride=8), :] for k in range(2)], axis=1)

        return jnp.concatenate([whole(near_ref), whole(far_ref)], axis=0)

    def influence(entry):
        square = column_ref[0] + (row_ref[0] + line_ref[0, entry])
        value = column_ref[1] * (row_ref[1] * line_ref[1, entry]) / jnp.where(square > 0, square, 1.0)
        return jnp.where(square > 0, value, 0.0)

    energy = jnp.zeros((KX, KY), f32)
    for plane in range(4):
        real, imag = times_x(plane_of(main_ref, far_ref, plane), plane_of(main_ref, far_ref, plane + 4))
        kernel = influence(me * 4 + plane)
        if plane == 0:
            mine = me == 0
            other = influence(KZ // 2)
            share = jnp.where(mine, 0.5 * (kernel + other), kernel)
            cross = jnp.where(mine, 0.5 * (kernel - other), 0.0)
            twin_real, twin_imag = times_x(
                plane_of(twin_ref, far_twin_ref, 0), plane_of(twin_ref, far_twin_ref, 4)
            )
            out_real = share * real + cross * twin_real
            out_imag = share * imag + cross * twin_imag
            energy = energy + jnp.where(mine, 0.5, 1.0) * (real * out_real + imag * out_imag)
        else:
            out_real = kernel * real
            out_imag = kernel * imag
            energy = energy + (real * out_real + imag * out_imag)
        real, imag = times_x(out_real, -out_imag)
        for k in range(2):
            side = slice(k * LANES, (k + 1) * LANES)
            main_ref[k, pl.ds(plane, near, stride=8), :] = real[:near, side]
            main_ref[k, pl.ds(plane + 4, near, stride=8), :] = -imag[:near, side]
            far_out_ref[k, pl.ds(plane, KX - near, stride=8), :] = real[near:, side]
            far_out_ref[k, pl.ds(plane + 4, KX - near, stride=8), :] = -imag[near:, side]

    total = jnp.sum(jnp.sum(energy, axis=0, keepdims=True), axis=1, keepdims=True)
    energy_ref[...] = jnp.broadcast_to(total, (8, LANES))
    backward_y(main_ref, y_high_ref, y_low_ref, out_ref, pens, width, out_ref.shape[2])


def plane_tables(block_x):
    angle = angles(np.arange(KY), np.arange(KY), KY)
    tables_y = table_halves(np.concatenate([np.cos(angle), np.sin(angle)], axis=1))
    order = np.arange(KX).reshape(KX // block_x, 2, block_x // 2).transpose(1, 0, 2).reshape(-1)
    angle = angles(order, order, KX)
    cos_x, sin_x = np.cos(angle), np.sin(angle)
    tables_x = table_halves(np.concatenate([cos_x, sin_x], axis=1))
    square_x, factor_x = np_line(KX)
    square_y, factor_y = np_line(KY)
    square_z, factor_z = np_line(KZ)
    factor_z = factor_z / (math.pi * KX * KY * KZ)
    column = jnp.asarray(np.float32(np.stack([square_x[order], factor_x[order]])))[:, :, None]
    row = jnp.asarray(np.float32(np.stack([square_y, factor_y])))[:, None, :]
    line = jnp.asarray(np.float32(np.stack([square_z, factor_z])))
    return tables_y, tables_x, column, row, line


def by_halves(atoms, slots, groups, block_x, block_y):
    groups_all, pens = lax.axis_size("grp"), lax.axis_size("pen")
    devices = groups_all * pens
    half = block_x // 2
    lines = half * block_y
    cut = (half - SPAN) // 2
    tiles_x = block_x // 2
    late = tiles_x - 4
    inner = groups - 1
    forward, back = z_table(devices)
    forward, back = table_halves(forward), table_halves(back.reshape(KZ, KZ))
    tables_y, tables_x, column, row, line = plane_tables(block_x)
    me = lax.axis_index(("grp", "pen")).reshape(1)
    sizes = (slots, groups, block_y)
    axes = ("grp", "pen")
    def exchange(spectral):
        return lax.all_to_all(spectral.reshape(devices, 8, -1), axes, 0, 0, tiled=True)

    edge_y = 8 * inner
    rim_pieces = [
        (0, block_x, block_y, block_y + 8),
        (block_x, block_x + REACH, 0, block_y), (block_x, block_x + REACH, block_y, block_y + 8),
    ]
    carried = [(0, half, edge_y, block_y), (half, block_x, edge_y, block_y), (2 * late, block_x, 0, edge_y)]
    ranges = [(0, tiles_x, inner, groups), (late, tiles_x, 0, inner)]
    rim_y, rim_x, corner, near_edge, far_edge, end = spread_charges(
        atoms, *sizes, ranges, rim_pieces + carried, [stored] * 4 + [kept] * 2
    )
    rim_y = shifted(rim_y, "pen", 1)
    rim_x = shifted(rim_x, "grp", 1)
    corner = shifted_both(corner, 1)
    pieces = [(half, block_x, 0, block_y), (2 * cut, half, 0, block_y)]
    atoms = [atoms[0], *resident(atoms[1:3]), *atoms[3:]]
    core, over = spread_charges(
        atoms, *sizes, [(cut, late, 0, inner)], pieces, [kept, stored], carried[1:], resident([far_edge, end])
    )
    far = forward_z(core, (rim_y,), *forward, half)
    over, far, rim_x, corner = lax.optimization_barrier((over, far, rim_x, corner))
    far = exchange(far)
    core, = spread_charges(
        atoms, *sizes, [(0, cut, 0, inner)], [(0, half, 0, block_y)], [kept],
        [pieces[1], (0, half, edge_y, block_y)], apart([over, near_edge]),
    )
    near = exchange(forward_z(core, (rim_y, rim_x, corner), *forward, 0))

    part = stored((2, KX // 2 * 8, LANES))
    far, far_twin = pl.pallas_call(
        functools.partial(planes_first_body, pens=pens, width=block_y),
        out_shape=[part, part],
        in_specs=[vmem] * 3,
        compiler_params=room,
        out_specs=[vmem] * 2,
        name="planes_first",
    )(*resident([far]), *apart(tables_y))
    near, far, energy = pl.pallas_call(
        functools.partial(planes_body, pens=pens, width=block_y),
        out_shape=[
            kept((devices, 8, lines)), part, stored((8, LANES)),
        ],
        in_specs=[smem, smem] + [vmem] * 9,
        compiler_params=room,
        out_specs=[vmem] * 3,
        scratch_shapes=[pltpu.VMEM(part.shape, f32)] * 2,
        name="planes",
    )(me, *apart([line]), *resident([near]), *apart([far, far_twin, *tables_y, *tables_x, column, row]))
    near = exchange(near)
    far = pl.pallas_call(
        functools.partial(planes_last_body, pens=pens, width=block_y, lines=lines),
        out_shape=kept((devices, 8, lines + LANES)),
        in_specs=[vmem] * 4,
        compiler_params=room,
        out_specs=vmem,
        name="planes_last",
    )(*apart([far, energy, *tables_y]))
    far = exchange(far)
    edges = [(REACH, block_y, KZ), (REACH, 8, KZ), (half - 2 * cut, block_y, KZ)]
    near, near_y, rim_x, corner, over = backward_z(near.reshape(KZ, -1), *back, half, block_y, edges)
    near_y = shifted(near_y, "pen", -1)
    rim_x = shifted(rim_x, "grp", -1)
    corner = shifted_both(corner, -1)
    pieces = [(0, 0, 0), (0, block_y, 0)]
    first = interpolate(
        atoms, *sizes, [(0, cut, 0, groups)], pieces, resident([near, near_y]), (0, cut), stored
    )
    far, first, rim_x, corner = lax.optimization_barrier((far, first, rim_x, corner))
    far, far_y, parts = backward_z(far.reshape(KZ, -1), *back, half, block_y, [], 1.0 / (devices * atoms[3].size))
    moved_y = shifted(far_y, "pen", -1)
    pieces = [(2 * cut, 0, 0), (half, 0, 0), (block_x, 0, 0)]
    over, = apart([over])
    far, rim_x, corner, near_y = resident([far, rim_x, corner, near_y])
    fields = (over, far, rim_x)
    second = interpolate(
        atoms, *sizes, [(cut, tiles_x, 0, inner)], pieces, fields, (cut, tiles_x), kept
    )
    pieces += [(0, block_y, 2 * cut), (half, block_y, 0), (block_x, block_y, 0)]
    fields += (near_y, *resident([moved_y]), corner)
    forces = interpolate(
        atoms, *sizes, [(cut, tiles_x, inner, groups)], pieces, fields, (0, tiles_x), stored,
        (*apart([first]), *resident([second])),
    )
    return forces, parts.reshape(())


def by_pencils(atoms, slots, groups, block_x, block_y):
    sizes = (slots, groups, block_y)
    ranges = [(0, block_x // 2, 0, groups)]
    pieces = [
        (0, block_x, 0, block_y), (0, block_x, block_y, block_y + 8),
        (block_x, block_x + REACH, 0, block_y), (block_x, block_x + REACH, block_y, block_y + 8),
    ]
    core, rim_y, rim_x, corner = spread_charges(atoms, *sizes, ranges, pieces, [stored] * 4)
    rims = (shifted(rim_y, "pen", 1), shifted(rim_x, "grp", 1), shifted_both(corner, 1))
    grid = core.at[:, :8].add(rims[0]).at[:REACH].add(rims[1]).at[:REACH, :8].add(rims[2])
    core, share = spectrum_pen_first(grid, block_x, block_y)
    rims = (shifted(core[:, :8], "pen", -1), shifted(core[:REACH], "grp", -1), shifted_both(core[:REACH, :8], -1))
    pieces = [(0, 0, 0), (0, block_y, 0), (block_x, 0, 0), (block_x, block_y, 0)]
    forces = interpolate(atoms, *sizes, ranges, pieces, (core, *rims), (0, block_x // 2), stored)
    total = lax.psum(share, ("grp", "pen"))
    return forces, total / (atoms[3].size * lax.axis_size("grp") * lax.axis_size("pen"))


def modulus(index, length):
    coeffs = (1.0 / 120.0, 26.0 / 120.0, 66.0 / 120.0, 26.0 / 120.0, 1.0 / 120.0)
    real_part = 0.0
    imag_part = 0.0
    for j in range(5):
        angle = (index * j % length).astype(jnp.float32) * (2.0 * math.pi / length)
        real_part = real_part + coeffs[j] * jnp.cos(angle)
        imag_part = imag_part + coeffs[j] * jnp.sin(angle)
    return real_part * real_part + imag_part * imag_part


def influence(index_x, index_y, index_z):
    freq_x = jnp.where(2 * index_x < KX, index_x, index_x - KX).astype(jnp.float32) / KX
    freq_y = jnp.where(2 * index_y < KY, index_y, index_y - KY).astype(jnp.float32) / KY
    freq_z = jnp.where(2 * index_z < KZ, index_z, index_z - KZ).astype(jnp.float32) / KZ
    square = freq_x * freq_x + freq_y * freq_y + freq_z * freq_z
    safe = jnp.where(square > 0, square, 1.0)
    volume = float(KX * KY * KZ)
    value = jnp.exp(-math.pi**2 * safe / ewald_split**2) / (math.pi * volume * safe)
    value = value / (modulus(index_x, KX) * modulus(index_y, KY) * modulus(index_z, KZ))
    return jnp.where(square > 0, value, 0.0)


def dft_tables(length):
    index = jnp.arange(length, dtype=jnp.int32)
    angle = (index[:, None] * index[None, :] % length).astype(jnp.float32) * (
        2.0 * math.pi / length
    )
    return (jnp.cos(angle), jnp.sin(angle))


def z_slots(groups):
    planes = KZ // (2 * groups) + 1
    owner = jnp.arange(groups, dtype=jnp.int32)[:, None]
    within = jnp.arange(planes, dtype=jnp.int32)[None, :]
    ordinary = owner * (planes - 1) + within
    frequency = jnp.where(within < planes - 1, ordinary, jnp.where(owner == 0, KZ // 2, 0))
    plane_weight = jnp.where(
        within < planes - 1, jnp.where(frequency == 0, 1.0, 2.0), jnp.where(owner == 0, 1.0, 0.0)
    )
    frequency = frequency.reshape(-1)
    plane_weight = plane_weight.reshape(-1).astype(jnp.float32)
    position = jnp.arange(KZ, dtype=jnp.int32)
    angle = (frequency[:, None] * position[None, :] % KZ).astype(jnp.float32) * (2.0 * math.pi / KZ)
    usable = (plane_weight > 0).astype(jnp.float32)[:, None]
    return (planes, frequency, plane_weight, jnp.cos(angle) * usable, jnp.sin(angle) * usable)


def forward_complex(data, cos_table, sin_table, shape, axis):
    direct = jnp.dot(cos_table, data, precision=highest).reshape(shape)
    other = jnp.dot(sin_table, data, precision=highest).reshape(shape)
    real_part = jnp.take(direct, 0, axis=axis) + jnp.take(other, 1, axis=axis)
    imag_part = jnp.take(direct, 1, axis=axis) - jnp.take(other, 0, axis=axis)
    return (real_part, imag_part)


def inverse_complex(data, cos_table, sin_table, shape, axis):
    direct = jnp.dot(cos_table, data, precision=highest).reshape(shape)
    other = jnp.dot(sin_table, data, precision=highest).reshape(shape)
    real_part = jnp.take(direct, 0, axis=axis) - jnp.take(other, 1, axis=axis)
    imag_part = jnp.take(other, 0, axis=axis) + jnp.take(direct, 1, axis=axis)
    return (real_part, imag_part)


def spectrum_pen_first(grid, block_x, block_y):
    cos_x, sin_x = dft_tables(KX)
    cos_y, sin_y = dft_tables(KY)
    planes, frequency, plane_weight, cos_z, sin_z = z_slots(lax.axis_size("pen"))
    slot_total = cos_z.shape[0]
    lines = KY // lax.axis_size("grp")
    real_z = jnp.einsum("xyz,kz->ykx", grid, cos_z, precision=highest)
    imag_z = -jnp.einsum("xyz,kz->ykx", grid, sin_z, precision=highest)
    outgoing = jnp.stack([real_z, imag_z], axis=2).reshape(block_y, slot_total * 2 * block_x)
    columns = lax.all_to_all(outgoing, "pen", split_axis=1, concat_axis=0, tiled=True)
    real_y, imag_y = forward_complex(columns, cos_y, sin_y, (KY, planes, 2, block_x), 2)
    sectioned = jnp.transpose(jnp.stack([real_y, imag_y], axis=-1), (2, 0, 1, 3)).reshape(
        block_x, KY * planes * 2
    )
    rows = lax.all_to_all(sectioned, "grp", split_axis=1, concat_axis=0, tiled=True)
    real_x, imag_x = forward_complex(rows, cos_x, sin_x, (KX, lines, planes, 2), 3)
    first = lax.axis_index("pen") * planes
    index_x = jnp.arange(KX, dtype=jnp.int32)[:, None, None]
    index_y = lax.axis_index("grp") * lines + jnp.arange(lines, dtype=jnp.int32)[None, :, None]
    index_z = lax.dynamic_slice_in_dim(frequency, first, planes)[None, None, :]
    local_weight = lax.dynamic_slice_in_dim(plane_weight, first, planes)[None, None, :]
    kernel = influence(index_x, index_y, index_z)
    spectral = 0.5 * jnp.sum(local_weight * kernel * (real_x * real_x + imag_x * imag_x))
    scaled = jnp.stack([kernel * real_x, kernel * imag_x], axis=-1).reshape(KX, lines * planes * 2)
    real_b, imag_b = inverse_complex(scaled, cos_x, sin_x, (KX, lines, planes, 2), 3)
    returning = jnp.stack([real_b, imag_b], axis=-1).reshape(KX, lines * planes * 2)
    rows_home = lax.all_to_all(returning, "grp", split_axis=0, concat_axis=1, tiled=True)
    rows_home = jnp.transpose(rows_home.reshape(block_x, KY, planes, 2), (1, 2, 3, 0)).reshape(
        KY, planes * 2 * block_x
    )
    real_c, imag_c = inverse_complex(rows_home, cos_y, sin_y, (KY, planes, 2, block_x), 2)
    leaving = jnp.stack([real_c, imag_c], axis=2).reshape(KY, planes * 2 * block_x)
    home = lax.all_to_all(leaving, "pen", split_axis=0, concat_axis=1, tiled=True).reshape(
        block_y, slot_total, 2, block_x
    )
    potential = jnp.einsum(
        "ykx,kz->xyz", home[:, :, 0], plane_weight[:, None] * cos_z, precision=highest
    )
    potential = potential - jnp.einsum(
        "ykx,kz->xyz", home[:, :, 1], plane_weight[:, None] * sin_z, precision=highest
    )
    return (potential, spectral)


def local(cell_offsets, cell_z, frac, charges, tile_counts):
    groups_all, pens = lax.axis_size("grp"), lax.axis_size("pen")
    devices = groups_all * pens
    block_x = KX // groups_all
    block_y = KY // pens
    slots = charges.shape[0] // tile_counts.shape[0]
    groups = block_y // 2 * slots // (2 * LANES)
    lines = charges.shape[0] // LANES
    slot_arrays = [frac, cell_offsets, cell_z.reshape(lines, LANES), charges.reshape(lines, LANES)]
    atoms = apart([tile_counts, *slot_arrays])
    if KZ == 8 * devices and 4 * block_y == LANES and pens == 8 and block_x % 16 == 0:
        return by_halves(atoms, slots, groups, block_x, block_y)
    return by_pencils(atoms, slots, groups, block_x, block_y)


def solution(mesh):
    in_specs = (
        P(None, ("grp", "pen")),
        P(("grp", "pen")),
        P(None, ("grp", "pen")),
        P(("grp", "pen")),
        P(("grp", "pen")),
    )
    out_specs = (P(None, ("grp", "pen")), P())
    return jax.shard_map(local, mesh=mesh, in_specs=in_specs, out_specs=out_specs, check_vma=False)
```

```python
import functools
import math

import jax
import jax.numpy as jnp
import numpy as np
from jax import lax
from jax.experimental import pallas as pl
from jax.experimental.pallas import tpu as pltpu
from jax.sharding import PartitionSpec as P

KX = 256
KY = 256
KZ = 256
LANES = 128
ROWS = 16
SPAN = 7
REACH = 5

ewald_split = 0.6
highest = lax.Precision.HIGHEST
f32 = jnp.float32
bf16 = jnp.bfloat16


def shifted(block, axis, distance):
    devices = range(lax.axis_size(axis))
    route = [((i - distance) % len(devices), i) for i in devices]
    return lax.ppermute(block, axis, route)


def shifted_both(block, distance):
    groups, pens = lax.axis_size("grp"), lax.axis_size("pen")
    route = []
    for g in range(groups):
        for p in range(pens):
            source = ((g - distance) % groups) * pens + (p - distance) % pens
            route.append((source, g * pens + p))
    return lax.ppermute(block, ("grp", "pen"), route)


def halves(value):
    high = value.astype(bf16)
    low = (value - high.astype(f32)).astype(bf16)
    return high, low


def table_halves(table):
    table = jnp.asarray(np.asarray(table, np.float32))
    return halves(table)


def dot(left, right, dims):
    return lax.dot_general(left, right, (dims, ((), ())), preferred_element_type=f32)


NN = ((1,), (0,))
NT = ((1,), (1,))


def spline_rows(x):
    values = [jnp.ones_like(x)]
    fifth = None
    for order in range(2, 7):
        nxt = []
        for j in range(order):
            term = None
            if j >= 1:
                term = values[j - 1] * (x + float(order - 1 - j))
            if j <= order - 2:
                other = values[j] * (float(1 + j) - x)
                term = other if term is None else term + other
            nxt.append(term)
        if order == 5:
            fifth = [v * (1.0 / 24.0) for v in nxt]
        values = nxt
    thetas = [v * (1.0 / 120.0) for v in values]
    slopes = [-fifth[0]]
    for j in range(1, 5):
        slopes.append(fifth[j - 1] - fifth[j])
    slopes.append(fifth[4])
    return thetas, slopes


def placed(rows, offset):
    out = []
    zero = jnp.zeros_like(rows[0])
    for i in range(SPAN):
        here = rows[i] if i <= 5 else zero
        before = rows[i - 1] if i >= 1 else zero
        out.append(jnp.where(offset == 0, here, before))
    return out


def spread_out(row):
    return jnp.broadcast_to(row, (ROWS, row.shape[-1]))


def group_places(step, ranges):
    places = []
    for k in range(4):
        index = step * 4 + k
        passed = 0
        row = col = 0
        for first, last, low, high in ranges:
            width = high - low
            inside = index - passed
            a, g = first + inside // width, low + inside % width
            row, col = (a, g) if passed == 0 else (jnp.where(inside >= 0, a, row), jnp.where(inside >= 0, g, col))
            passed += (last - first) * width
        places.append((row, col))
    return places


def step_count(ranges):
    return sum((last - first) * (high - low) for first, last, low, high in ranges) // 4


def live_part(charge, counts_ref, lines, slots):
    per_row = LANES // slots
    row_at = lax.broadcasted_iota(jnp.int32, (8, LANES), 0)
    lane_at = lax.broadcasted_iota(jnp.int32, (8, LANES), 1)
    tile_at = row_at * per_row + lane_at // slots
    count = jnp.zeros((8, LANES), jnp.int32)
    for r, line in enumerate(lines):
        for k in range(per_row):
            count = jnp.where(tile_at == r * per_row + k, counts_ref[line * per_row + k], count)
    return jnp.where(lane_at % slots < count, charge, 0.0)


def step_atoms(places, refs, slots, groups):
    frac_ref, offs_ref, z_ref, q_ref = refs[-4:]
    per_row = LANES // slots
    lines = [(a * groups + g) * 2 + half for a, g in places for half in range(2)]

    def wide(ref, d):
        rows = [ref[d : d + 1, pl.ds(pl.multiple_of(line * LANES, LANES), LANES)] for line in lines]
        return jnp.concatenate(rows, axis=0)

    def tall(ref):
        return jnp.concatenate([ref[pl.ds(line, 1), :] for line in lines], axis=0)

    row_at = lax.broadcasted_iota(jnp.int32, (8, LANES), 0)
    lane_at = lax.broadcasted_iota(jnp.int32, (8, LANES), 1)
    charge = tall(q_ref)
    if len(refs) == 5:
        charge = live_part(charge, refs[0], lines, slots)
    tile_in_group = (row_at % 2) * per_row + lane_at // slots
    fracs = [wide(frac_ref, d) for d in range(3)]
    return fracs, wide(offs_ref, 0), wide(offs_ref, 1) + 2 * tile_in_group, tall(z_ref), charge, lines


def keep_rows(tab_ref, lists):
    for q, rows in enumerate(lists):
        for j, value in enumerate(rows):
            tab_ref[pl.ds(64 * q + 8 * j, 8), :] = value


def clear_rows(tab_ref):
    tab_ref[...] = jnp.zeros_like(tab_ref)


def by_distance(distance, tab_ref, q, row):
    table = tab_ref[pl.ds(64 * q + row, 8, stride=8), :]
    at = jnp.minimum(distance & 15, 7)
    return jnp.concatenate(
        [jnp.take_along_axis(table, at[k : k + 8], axis=0, mode="promise_in_bounds") for k in (0, 8)], axis=0
    )


def z_parts(zcell, row, tab_ref, lists):
    cell = spread_out(zcell[row : row + 1])
    at = lax.broadcasted_iota(jnp.int32, (ROWS, LANES), 0)
    ahead = (at - cell) & (ROWS - 1)
    block = ((cell + ahead) & (KZ - 1)) // ROWS
    weights = [by_distance(ahead, tab_ref, q, row) for q in lists]
    return block.astype(f32).astype(bf16), weights


def z_matrix(block, weight):
    zero = jnp.zeros_like(weight)
    return jnp.concatenate(
        [jnp.where(block == jnp.array(k, bf16), weight, zero) for k in range(KZ // ROWS)], axis=0
    )


def spread_body(*refs, slots, groups, ranges, base, pieces, carried, given, emit):
    atom_refs = refs[:given]
    acc_ref, tab_ref = refs[-2:]
    acc_ref[...] = jnp.zeros_like(acc_ref)
    clear_rows(tab_ref)
    for piece, ref in zip(carried, refs[given:]):
        low = (piece[0] - base, piece[2])
        acc_ref[low[0] : low[0] + ref.shape[0], low[1] : low[1] + ref.shape[1]] += ref[...]
    refs = refs[given + len(carried) :]
    at = lax.broadcasted_iota(jnp.int32, (ROWS, LANES), 0)

    def body(step, carry):
        places = group_places(step, ranges)
        fracs, offset_x, offset_y, zcell, charge, lines = step_atoms(places, atom_refs, slots, groups)
        theta_x, _ = spline_rows(fracs[0])
        theta_y, _ = spline_rows(fracs[1])
        theta_z, _ = spline_rows(fracs[2])
        theta_y = [t * charge for t in theta_y]
        weight_x = placed(theta_x, offset_x)
        keep_rows(tab_ref, [theta_z, theta_y])
        for k in range(4):
            blocks, zs, pairs = [], [], []
            for half in range(2):
                line = 2 * k + half
                row = slice(line, line + 1)
                block, (weight,) = z_parts(zcell, line, tab_ref, [0])
                blocks.append(block)
                zs.append(weight)
                weight_y = by_distance(at - spread_out(offset_y[row]), tab_ref, 1, line)
                pairs.append([spread_out(weight_x[i][row]) * weight_y for i in range(SPAN)])
            block = jnp.concatenate(blocks, axis=1)
            z_high, z_low = halves(jnp.concatenate(zs, axis=1))
            table_high = z_matrix(block, z_high)
            table_low = z_matrix(block, z_low)
            pair = jnp.concatenate(
                [jnp.concatenate([pairs[0][i], pairs[1][i]], axis=1) for i in range(SPAN)], axis=0
            )
            high, low = halves(pair)
            both = dot(jnp.concatenate([high, low], axis=0), table_high, NT)
            rest = dot(high, table_low, NT)
            total = both[: SPAN * ROWS] + both[SPAN * ROWS :] + rest
            a, g = places[k]
            where = (pl.ds(2 * a - base, SPAN), pl.ds(pl.multiple_of(8 * g, 8), ROWS))
            acc_ref[where[0], where[1], :] += total.reshape(SPAN, ROWS, KZ)
        return carry

    lax.fori_loop(0, step_count(ranges), body, 0)
    if emit:
        z_out_ref, live_ref = refs[len(pieces) : len(pieces) + 2]
        z_out_ref[...] = atom_refs[3][...]

        def live_body(step, carry):
            rows = pl.ds(pl.multiple_of(8 * step, 8), 8)
            lines = [8 * step + r for r in range(8)]
            live_ref[rows, :] = live_part(atom_refs[4][rows, :], atom_refs[0], lines, slots)
            return carry

        lax.fori_loop(0, live_ref.shape[0] // 8, live_body, 0)
    for piece, ref in zip(pieces, refs):
        ref[...] = acc_ref[piece[0] - base : piece[1] - base, piece[2] : piece[3], :]


vmem = pl.BlockSpec(memory_space=pltpu.VMEM)
room = pltpu.CompilerParams(vmem_limit_bytes=28 * 1024 * 1024)


def resident(values):
    return [pltpu.with_memory_space_constraint(value, pltpu.VMEM) for value in values]


def apart(values):
    return [pltpu.with_memory_space_constraint(value, pltpu.HBM) for value in values]


def kept(shape):
    return pltpu.VMEM(shape, f32)


def stored(shape):
    return pltpu.HBM(shape, f32)


smem = pl.BlockSpec(memory_space=pltpu.SMEM)


def spread_charges(atoms, slots, groups, block_y, ranges, pieces, holds, carried=(), fields=(), emit=False):
    base = min([2 * r[0] for r in ranges] + [p[0] for p in pieces + list(carried)])
    top = max([2 * r[1] + REACH for r in ranges] + [p[1] for p in pieces + list(carried)])
    body = functools.partial(
        spread_body, slots=slots, groups=groups, ranges=ranges, base=base, pieces=pieces, carried=carried,
        given=len(atoms), emit=emit,
    )
    shapes = [(p[1] - p[0], p[3] - p[2], KZ) for p in pieces]
    shapes = [hold(s) for hold, s in zip(holds, shapes)]
    if emit:
        shapes += [pltpu.VMEM(atoms[3].shape, jnp.int32), kept(atoms[4].shape)]
    return pl.pallas_call(
        body,
        out_shape=shapes,
        in_specs=[smem] * (len(atoms) - 4) + [vmem] * (4 + len(fields)),
        compiler_params=room,
        out_specs=[vmem] * len(shapes),
        scratch_shapes=[pltpu.VMEM((top - base, block_y + 8, KZ), f32), pltpu.VMEM((128, LANES), f32)],
        name="spread",
    )(*atoms, *fields)


def interp_body(*refs, slots, groups, ranges, base, pieces, before, first):
    atom_refs = refs[:5]
    out_ref, pot_ref, tab_ref = refs[-3:]
    clear_rows(tab_ref)
    refs = refs[5:]
    for (low_x, low_y, skip), ref in zip(pieces, refs):
        tall, wide = ref.shape[0] - skip, ref.shape[1]
        pot_ref[low_x + skip - base : low_x + skip - base + tall, low_y : low_y + wide, :] = ref[skip:]
    for k in range(before):
        earlier_ref = refs[len(pieces) + k]
        start = earlier_ref.shape[1] * k if k == 0 else out_ref.shape[1] - earlier_ref.shape[1]
        out_ref[:, start : start + earlier_ref.shape[1]] = earlier_ref[...]
    at = lax.broadcasted_iota(jnp.int32, (ROWS, LANES), 0)
    height = SPAN * ROWS

    def body(step, carry):
        places = group_places(step, ranges)
        fracs, offset_x, offset_y, zcell, charge, lines = step_atoms(places, atom_refs, slots, groups)
        theta_x, slope_x = spline_rows(fracs[0])
        theta_y, slope_y = spline_rows(fracs[1])
        theta_z, slope_z = spline_rows(fracs[2])
        theta_y = [t * -charge for t in theta_y]
        slope_y = [t * -charge for t in slope_y]
        weight_x = placed(theta_x, offset_x)
        grade_x = placed(slope_x, offset_x)
        keep_rows(tab_ref, [theta_z, slope_z, theta_y, slope_y])
        for k in range(4):
            blocks, zs, gs = [], [], []
            for half in range(2):
                block, (weight, grade) = z_parts(zcell, 2 * k + half, tab_ref, [0, 1])
                blocks.append(block)
                zs.append(weight)
                gs.append(grade)
            block = jnp.concatenate(blocks, axis=1)
            z_high, z_low = halves(jnp.concatenate(zs, axis=1))
            g_high, g_low = halves(jnp.concatenate(gs, axis=1))
            a, g = places[k]
            slab = pot_ref[pl.ds(2 * a - base, SPAN), pl.ds(pl.multiple_of(8 * g, 8), ROWS), :]
            high, low = halves(slab.reshape(height, KZ))
            stacked = jnp.concatenate([high, low], axis=0)
            main = dot(stacked, z_matrix(block, z_high), NN)
            main = main[:height] + main[height:] + dot(high, z_matrix(block, z_low), NN)
            tilt = dot(stacked, z_matrix(block, g_high), NN)
            tilt = tilt[:height] + tilt[height:] + dot(high, z_matrix(block, g_low), NN)
            for half in range(2):
                row = slice(2 * k + half, 2 * k + half + 1)
                lanes = slice(half * LANES, (half + 1) * LANES)
                away = at - spread_out(offset_y[row])
                weight_y = by_distance(away, tab_ref, 2, 2 * k + half)
                grade_y = by_distance(away, tab_ref, 3, 2 * k + half)
                plain = steep = tilted = 0.0
                for i in range(SPAN):
                    part = slice(i * ROWS, (i + 1) * ROWS)
                    wide = spread_out(weight_x[i][row])
                    plain = plain + wide * main[part, lanes]
                    tilted = tilted + wide * tilt[part, lanes]
                    steep = steep + spread_out(grade_x[i][row]) * main[part, lanes]
                forces = [
                    jnp.sum(steep * weight_y, axis=0, keepdims=True),
                    jnp.sum(plain * grade_y, axis=0, keepdims=True),
                    jnp.sum(tilted * weight_y, axis=0, keepdims=True),
                ]
                start = (lines[2 * k + half] - first) * LANES
                out_ref[:, pl.ds(pl.multiple_of(start, LANES), LANES)] = jnp.concatenate(forces, axis=0)
        return carry

    lax.fori_loop(0, step_count(ranges), body, 0)


def interpolate(atoms, slots, groups, block_y, ranges, pieces, fields, rows, hold, earlier=()):
    base = min(2 * r[0] for r in ranges)
    line = 2 * groups
    body = functools.partial(
        interp_body, slots=slots, groups=groups, ranges=ranges, base=base, pieces=pieces,
        before=len(earlier), first=rows[0] * line,
    )
    height = max(max(2 * r[1] + REACH for r in ranges), max(p[0] + f.shape[0] for p, f in zip(pieces, fields))) - base
    return pl.pallas_call(
        body,
        out_shape=hold((3, (rows[1] - rows[0]) * line * LANES)),
        in_specs=[smem] + [vmem] * (4 + len(fields) + len(earlier)),
        compiler_params=room,
        out_specs=vmem,
        scratch_shapes=[pltpu.VMEM((height, block_y + 8, KZ), f32), pltpu.VMEM((256, LANES), f32)],
        name="interpolate",
    )(*atoms, *fields, *earlier)


def angles(left, right, length):
    return (np.outer(left, right) % length) * (2.0 * math.pi / length)


def np_modulus(length):
    index = np.arange(length)
    coeffs = (1.0 / 120.0, 26.0 / 120.0, 66.0 / 120.0, 26.0 / 120.0, 1.0 / 120.0)
    total = 0.0
    for j in range(5):
        total = total + coeffs[j] * np.exp(2j * math.pi * ((index * j) % length) / length)
    return np.abs(total) ** 2


def np_line(length):
    index = np.arange(length)
    freq = np.where(2 * index < length, index, index - length) / length
    square = freq * freq
    return square, np.exp(-(math.pi**2) * square / ewald_split**2) / np_modulus(length)


def z_table(devices):
    per = KZ // 2 // devices
    position = np.arange(KZ)
    forward, back = [], []
    for device in range(devices):
        for imaginary in range(2):
            for plane in range(device * per, (device + 1) * per):
                wave = 2.0 * math.pi * ((plane * position) % KZ) / KZ
                if plane == 0:
                    row = np.where(position % 2 == 0, 1.0, -1.0) if imaginary else np.ones(KZ)
                    forward.append(row)
                    back.append(row)
                else:
                    row = -np.sin(wave) if imaginary else np.cos(wave)
                    forward.append(row)
                    back.append(2.0 * row)
    return np.stack(forward), np.stack(back)


def forward_z_body(core_ref, rim_y_ref, *refs, chunk, first):
    out_ref = refs[-1]
    high = refs[-3][...]
    low = refs[-2][...]
    sides = refs[:-3]
    block_x, block_y = core_ref.shape[:2]
    stacked = jnp.concatenate([high, low], axis=0)
    size = high.shape[0]
    for start in range(0, block_x, chunk):
        part = core_ref[start : start + chunk]
        edge = part[:, :8] + rim_y_ref[first + start : first + start + chunk]
        rest = part[:, 8:]
        if sides and start < REACH:
            count = min(REACH - start, chunk)
            side = sides[0][start : start + count]
            fix = side[:, :8] + sides[1][start : start + count]
            edge = jnp.concatenate([edge[:count] + fix, edge[count:]], axis=0)
            rest = jnp.concatenate([rest[:count] + side[:, 8:], rest[count:]], axis=0)
        part = jnp.concatenate([edge, rest], axis=1).reshape(chunk * block_y, KZ)
        part_high, part_low = halves(part)
        both = dot(stacked, part_high, NT)
        total = both[:size] + both[size:] + dot(high, part_low, NT)
        out_ref[:, start * block_y : (start + chunk) * block_y] = total


def forward_z(core, rims, high, low, first):
    block_x, block_y = core.shape[:2]
    chunk = 256 // block_y
    return pl.pallas_call(
        functools.partial(forward_z_body, chunk=chunk, first=first),
        out_shape=kept((KZ, block_x * block_y)),
        in_specs=[vmem] * (3 + len(rims)),
        compiler_params=room,
        out_specs=vmem,
        name="forward_z",
    )(*resident([core, *rims]), high, low)


def backward_z_body(in_ref, high_ref, low_ref, core_ref, rim_y_ref, *refs, chunk, scale):
    block_x, block_y = core_ref.shape[:2]
    high = high_ref[...]
    low = low_ref[...]
    for start in range(0, block_x, chunk):
        part = in_ref[:, start * block_y : (start + chunk) * block_y].T
        part_high, part_low = halves(part)
        size = part.shape[0]
        both = dot(jnp.concatenate([part_high, part_low], axis=0), high, NN)
        total = both[:size] + both[size:] + dot(part_high, low, NN)
        total = total.reshape(chunk, block_y, KZ)
        core_ref[start : start + chunk] = total
        rim_y_ref[start : start + chunk] = total[:, :8]
        if len(refs) == 3:
            if start < REACH:
                count = min(REACH - start, chunk)
                refs[0][start : start + count] = total[:count]
                refs[1][start : start + count] = total[:count, :8]
            over = block_x - refs[2].shape[0]
            if start >= over:
                refs[2][start - over : start - over + chunk] = total
    if len(refs) == 1:
        tail = in_ref[:, block_x * block_y :]
        refs[0][0] = jnp.max(jnp.sum(tail.reshape(-1, 8, LANES), axis=0)) * scale


def backward_z(spectral, high, low, block_x, block_y, others, scale=None):
    chunk = 256 // block_y
    sent = [(block_x, 8, KZ)] + others
    total = [] if scale is None else [jax.ShapeDtypeStruct((1,), f32)]
    return pl.pallas_call(
        functools.partial(backward_z_body, chunk=chunk, scale=scale),
        out_shape=[kept((block_x, block_y, KZ))] + [stored(s) for s in sent] + total,
        in_specs=[vmem] * 3,
        compiler_params=room,
        out_specs=[vmem] * (1 + len(sent)) + [smem] * len(total),
        name="backward_z",
    )(*resident([spectral]), high, low)


def swap_blocks(parts, width):
    lane_at = lax.broadcasted_iota(jnp.int32, parts[0].shape, 1)
    first = lane_at < 2 * width
    even = (lane_at // width) % 2 == 0
    a, b, c, d = parts
    a, c = jnp.where(first, a, pltpu.roll(c, 2 * width, 1)), jnp.where(first, pltpu.roll(a, 2 * width, 1), c)
    b, d = jnp.where(first, b, pltpu.roll(d, 2 * width, 1)), jnp.where(first, pltpu.roll(b, 2 * width, 1), d)
    back = LANES - width
    a, b = jnp.where(even, a, pltpu.roll(b, width, 1)), jnp.where(even, pltpu.roll(a, back, 1), b)
    c, d = jnp.where(even, c, pltpu.roll(d, width, 1)), jnp.where(even, pltpu.roll(c, back, 1), d)
    return [a, b, c, d]


STEP = 256


def times_y(rows, y_high, y_low):
    high, low = halves(rows)
    size = rows.shape[0]
    both = dot(jnp.concatenate([high, low], axis=0), y_high, NN)
    total = both[:size] + both[size:] + dot(high, y_low, NN)
    turned = pltpu.roll(total[:, KY:].reshape(size // 8, 8, KY), 4, 1).reshape(size, KY)
    return total[:, :KY], turned


def row_sign():
    comp_at = lax.broadcasted_iota(jnp.int32, (STEP, KY), 0) % 8
    return jnp.where(comp_at < 4, 1.0, -1.0)


def forward_y(in_ref, y_high_ref, y_low_ref, main_ref, twin_ref, pens, width):
    y_high = y_high_ref[...]
    y_low = y_low_ref[...]
    sign = row_sign()
    per_step = STEP // 32
    spans = in_ref.shape[2] // LANES // per_step
    groups = in_ref.shape[0] // pens

    def body(step, carry):
        group = step // spans
        rows = []
        for k in range(per_step):
            at = (step % spans) * per_step + k
            lanes = pl.ds(pl.multiple_of(at * LANES, LANES), LANES)
            lower = swap_blocks([in_ref[group * pens + p, :, lanes] for p in range(4)], width)
            upper = swap_blocks([in_ref[group * pens + 4 + p, :, lanes] for p in range(4)], width)
            for low, up in zip(lower, upper):
                rows.append(jnp.concatenate([low, up], axis=1))
        plain, turned = times_y(jnp.concatenate(rows, axis=0), y_high, y_low)
        at = pl.ds(pl.multiple_of(step * STEP, STEP), STEP)
        main = plain + sign * turned
        twin = sign * plain - turned
        for k in range(2):
            side = slice(k * LANES, (k + 1) * LANES)
            main_ref[k, at, :] = main[:, side]
            twin_ref[k, at, :] = twin[:, side]
        return carry

    lax.fori_loop(0, groups * spans, body, 0)


def backward_y(main_ref, y_high_ref, y_low_ref, out_ref, pens, width, lines):
    y_high = y_high_ref[...]
    y_low = y_low_ref[...]
    sign = row_sign()
    per_step = STEP // 32
    spans = lines // LANES // per_step
    groups = out_ref.shape[0] // pens

    def body(step, carry):
        group = step // spans
        at = pl.ds(pl.multiple_of(step * STEP, STEP), STEP)
        joined = jnp.concatenate([main_ref[0, at, :], main_ref[1, at, :]], axis=1)
        plain, turned = times_y(joined, y_high, y_low)
        rows = plain - sign * turned
        for k in range(per_step):
            at = (step % spans) * per_step + k
            lanes = pl.ds(pl.multiple_of(at * LANES, LANES), LANES)
            pieces = [rows[(4 * k + j) * 8 : (4 * k + j + 1) * 8] for j in range(4)]
            lower = swap_blocks([piece[:, :LANES] for piece in pieces], width)
            upper = swap_blocks([piece[:, LANES:] for piece in pieces], width)
            for p in range(4):
                out_ref[group * pens + p, :, lanes] = lower[p]
                out_ref[group * pens + 4 + p, :, lanes] = upper[p]
        return carry

    lax.fori_loop(0, groups * spans, body, 0)


def planes_first_body(in_ref, y_high_ref, y_low_ref, main_ref, pair_ref, twin_ref, *, pens, width):
    forward_y(in_ref, y_high_ref, y_low_ref, main_ref, twin_ref, pens, width)
    count = twin_ref.shape[1] // 8
    for k in range(2):
        for part in range(2):
            pair_ref[k, part * count : (part + 1) * count, :] = twin_ref[k, pl.ds(4 * part, count, stride=8), :]


def planes_last_body(main_ref, energy_ref, y_high_ref, y_low_ref, out_ref, *, pens, width, lines):
    backward_y(main_ref, y_high_ref, y_low_ref, out_ref, pens, width, lines)
    out_ref[:, :, lines:] = jnp.broadcast_to(energy_ref[...].reshape(1, 8, LANES), (out_ref.shape[0], 8, LANES))


def planes_body(
    where_ref, line_ref, in_ref, far_ref, far_twin_ref, y_high_ref, y_low_ref, x_high_ref, x_low_ref,
    column_ref, row_ref, out_ref, far_out_ref, energy_ref, main_ref, twin_ref,
    *, pens, width,
):
    me = where_ref[0]
    forward_y(in_ref, y_high_ref, y_low_ref, main_ref, twin_ref, pens, width)
    near = main_ref.shape[1] // 8

    def times_x(real, imag):
        high, low = [
            jnp.concatenate(
                [jnp.concatenate([r, i], axis=1), jnp.concatenate([i, -r], axis=1)], axis=0
            )
            for r, i in zip(halves(real), halves(imag))
        ]
        x_high = x_high_ref[...]
        total = dot(x_high, high, NN) + dot(x_high, low, NN) + dot(x_low_ref[...], high, NN)
        return total[:, :KY], total[:, KY:]

    def plane_of(near_ref, far_ref, comp):
        def whole(ref):
            return jnp.concatenate([ref[k, pl.ds(comp, ref.shape[1] // 8, stride=8), :] for k in range(2)], axis=1)

        if far_ref is None:
            rows = slice(comp // 4 * (KX - near), (comp // 4 + 1) * (KX - near))
            far_rows = jnp.concatenate([far_twin_ref[k, rows, :] for k in range(2)], axis=1)
        else:
            far_rows = whole(far_ref)
        return jnp.concatenate([whole(near_ref), far_rows], axis=0)

    def influence(entry):
        square = column_ref[0] + (row_ref[0] + line_ref[0, entry])
        value = column_ref[1] * (row_ref[1] * line_ref[1, entry]) / jnp.where(square > 0, square, 1.0)
        return jnp.where(square > 0, value, 0.0)

    energy = jnp.zeros((KX, KY), f32)
    for plane in range(4):
        real, imag = times_x(plane_of(main_ref, far_ref, plane), plane_of(main_ref, far_ref, plane + 4))
        kernel = influence(me * 4 + plane)
        if plane == 0:
            mine = me == 0
            other = influence(KZ // 2)
            share = jnp.where(mine, 0.5 * (kernel + other), kernel)
            cross = jnp.where(mine, 0.5 * (kernel - other), 0.0)
            twin_real, twin_imag = times_x(plane_of(twin_ref, None, 0), plane_of(twin_ref, None, 4))
            out_real = share * real + cross * twin_real
            out_imag = share * imag + cross * twin_imag
            energy = energy + jnp.where(mine, 0.5, 1.0) * (real * out_real + imag * out_imag)
        else:
            out_real = kernel * real
            out_imag = kernel * imag
            energy = energy + (real * out_real + imag * out_imag)
        real, imag = times_x(out_real, -out_imag)
        for k in range(2):
            side = slice(k * LANES, (k + 1) * LANES)
            main_ref[k, pl.ds(plane, near, stride=8), :] = real[:near, side]
            main_ref[k, pl.ds(plane + 4, near, stride=8), :] = -imag[:near, side]
            far_out_ref[k, pl.ds(plane, KX - near, stride=8), :] = real[near:, side]
            far_out_ref[k, pl.ds(plane + 4, KX - near, stride=8), :] = -imag[near:, side]

    total = jnp.sum(jnp.sum(energy, axis=0, keepdims=True), axis=1, keepdims=True)
    energy_ref[...] = jnp.broadcast_to(total, (8, LANES))
    backward_y(main_ref, y_high_ref, y_low_ref, out_ref, pens, width, out_ref.shape[2])


def plane_tables(block_x):
    angle = angles(np.arange(KY), np.arange(KY), KY)
    tables_y = table_halves(np.concatenate([np.cos(angle), np.sin(angle)], axis=1))
    order = np.arange(KX).reshape(KX // block_x, 2, block_x // 2).transpose(1, 0, 2).reshape(-1)
    angle = angles(order, order, KX)
    cos_x, sin_x = np.cos(angle), np.sin(angle)
    tables_x = table_halves(np.concatenate([cos_x, sin_x], axis=1))
    square_x, factor_x = np_line(KX)
    square_y, factor_y = np_line(KY)
    square_z, factor_z = np_line(KZ)
    factor_z = factor_z / (math.pi * KX * KY * KZ)
    column = jnp.asarray(np.float32(np.stack([square_x[order], factor_x[order]])))[:, :, None]
    row = jnp.asarray(np.float32(np.stack([square_y, factor_y])))[:, None, :]
    line = jnp.asarray(np.float32(np.stack([square_z, factor_z])))
    return tables_y, tables_x, column, row, line


def by_halves(atoms, slots, groups, block_x, block_y):
    groups_all, pens = lax.axis_size("grp"), lax.axis_size("pen")
    devices = groups_all * pens
    half = block_x // 2
    lines = half * block_y
    cut = (half - SPAN) // 2
    tiles_x = block_x // 2
    late = tiles_x - 4
    inner = groups - 1
    forward, back = z_table(devices)
    forward, back = table_halves(forward), table_halves(back.reshape(KZ, KZ))
    tables_y, tables_x, column, row, line = plane_tables(block_x)
    me = lax.axis_index(("grp", "pen")).reshape(1)
    sizes = (slots, groups, block_y)
    axes = ("grp", "pen")
    def exchange(spectral):
        return lax.all_to_all(spectral.reshape(devices, 8, -1), axes, 0, 0, tiled=True)

    edge_y = 8 * inner
    rim_pieces = [
        (0, block_x, block_y, block_y + 8),
        (block_x, block_x + REACH, 0, block_y), (block_x, block_x + REACH, block_y, block_y + 8),
    ]
    carried = [(0, half, edge_y, block_y), (half, block_x, edge_y, block_y), (2 * late, block_x, 0, edge_y)]
    ranges = [(0, tiles_x, inner, groups), (late, tiles_x, 0, inner)]
    rim_y, rim_x, corner, near_edge, far_edge, end, z_kept, live = spread_charges(
        atoms, *sizes, ranges, rim_pieces + carried, [stored] * 4 + [kept] * 2, emit=True
    )
    rim_y = shifted(rim_y, "pen", 1)
    rim_x = shifted(rim_x, "grp", 1)
    corner = shifted_both(corner, 1)
    pieces = [(half, block_x, 0, block_y), (2 * cut, half, 0, block_y)]
    atoms = [atoms[0], *resident(atoms[1:3]), *atoms[3:]]
    core, over = spread_charges(
        [*atoms[1:3], *resident([z_kept, live])], *sizes, [(cut, late, 0, inner)], pieces, [kept, stored], carried[1:], resident([far_edge, end])
    )
    far = forward_z(core, (rim_y,), *forward, half)
    over, far, rim_x, corner = lax.optimization_barrier((over, far, rim_x, corner))
    far = exchange(far)
    core, = spread_charges(
        atoms, *sizes, [(0, cut, 0, inner)], [(0, half, 0, block_y)], [kept],
        [pieces[1], (0, half, edge_y, block_y)], apart([over, near_edge]),
    )
    near = exchange(forward_z(core, (rim_y, rim_x, corner), *forward, 0))

    part = stored((2, KX // 2 * 8, LANES))
    far, far_twin = pl.pallas_call(
        functools.partial(planes_first_body, pens=pens, width=block_y),
        out_shape=[part, stored((2, KX, LANES))],
        scratch_shapes=[pltpu.VMEM((2, KX // 2 * 8, LANES), f32)],
        in_specs=[vmem] * 3,
        compiler_params=room,
        out_specs=[vmem] * 2,
        name="planes_first",
    )(*resident([far]), *apart(tables_y))
    near, far, energy = pl.pallas_call(
        functools.partial(planes_body, pens=pens, width=block_y),
        out_shape=[
            kept((devices, 8, lines)), part, stored((8, LANES)),
        ],
        in_specs=[smem, smem] + [vmem] * 9,
        compiler_params=room,
        out_specs=[vmem] * 3,
        scratch_shapes=[pltpu.VMEM(part.shape, f32)] * 2,
        name="planes",
    )(me, *apart([line]), *resident([near]), *apart([far, far_twin, *tables_y, *tables_x, column, row]))
    near = exchange(near)
    far = pl.pallas_call(
        functools.partial(planes_last_body, pens=pens, width=block_y, lines=lines),
        out_shape=kept((devices, 8, lines + LANES)),
        in_specs=[vmem] * 4,
        compiler_params=room,
        out_specs=vmem,
        name="planes_last",
    )(*apart([far, energy, *tables_y]))
    far = exchange(far)
    edges = [(REACH, block_y, KZ), (REACH, 8, KZ), (half - 2 * cut, block_y, KZ)]
    near, near_y, rim_x, corner, over = backward_z(near.reshape(KZ, -1), *back, half, block_y, edges)
    near_y = shifted(near_y, "pen", -1)
    rim_x = shifted(rim_x, "grp", -1)
    corner = shifted_both(corner, -1)
    pieces = [(0, 0, 0), (0, block_y, 0)]
    first = interpolate(
        atoms, *sizes, [(0, cut, 0, groups)], pieces, resident([near, near_y]), (0, cut), stored
    )
    far, first, rim_x, corner = lax.optimization_barrier((far, first, rim_x, corner))
    far, far_y, parts = backward_z(far.reshape(KZ, -1), *back, half, block_y, [], 1.0 / (devices * atoms[3].size))
    moved_y = shifted(far_y, "pen", -1)
    pieces = [(2 * cut, 0, 0), (half, 0, 0), (block_x, 0, 0)]
    over, = apart([over])
    far, rim_x, corner, near_y = resident([far, rim_x, corner, near_y])
    fields = (over, far, rim_x)
    second = interpolate(
        atoms, *sizes, [(cut, tiles_x, 0, inner)], pieces, fields, (cut, tiles_x), kept
    )
    pieces += [(0, block_y, 2 * cut), (half, block_y, 0), (block_x, block_y, 0)]
    fields += (near_y, *resident([moved_y]), corner)
    forces = interpolate(
        atoms, *sizes, [(cut, tiles_x, inner, groups)], pieces, fields, (0, tiles_x), stored,
        (*apart([first]), *resident([second])),
    )
    return forces, parts.reshape(())


def by_pencils(atoms, slots, groups, block_x, block_y):
    sizes = (slots, groups, block_y)
    ranges = [(0, block_x // 2, 0, groups)]
    pieces = [
        (0, block_x, 0, block_y), (0, block_x, block_y, block_y + 8),
        (block_x, block_x + REACH, 0, block_y), (block_x, block_x + REACH, block_y, block_y + 8),
    ]
    core, rim_y, rim_x, corner = spread_charges(atoms, *sizes, ranges, pieces, [stored] * 4)
    rims = (shifted(rim_y, "pen", 1), shifted(rim_x, "grp", 1), shifted_both(corner, 1))
    grid = core.at[:, :8].add(rims[0]).at[:REACH].add(rims[1]).at[:REACH, :8].add(rims[2])
    core, share = spectrum_pen_first(grid, block_x, block_y)
    rims = (shifted(core[:, :8], "pen", -1), shifted(core[:REACH], "grp", -1), shifted_both(core[:REACH, :8], -1))
    pieces = [(0, 0, 0), (0, block_y, 0), (block_x, 0, 0), (block_x, block_y, 0)]
    forces = interpolate(atoms, *sizes, ranges, pieces, (core, *rims), (0, block_x // 2), stored)
    total = lax.psum(share, ("grp", "pen"))
    return forces, total / (atoms[3].size * lax.axis_size("grp") * lax.axis_size("pen"))


def modulus(index, length):
    coeffs = (1.0 / 120.0, 26.0 / 120.0, 66.0 / 120.0, 26.0 / 120.0, 1.0 / 120.0)
    real_part = 0.0
    imag_part = 0.0
    for j in range(5):
        angle = (index * j % length).astype(jnp.float32) * (2.0 * math.pi / length)
        real_part = real_part + coeffs[j] * jnp.cos(angle)
        imag_part = imag_part + coeffs[j] * jnp.sin(angle)
    return real_part * real_part + imag_part * imag_part


def influence(index_x, index_y, index_z):
    freq_x = jnp.where(2 * index_x < KX, index_x, index_x - KX).astype(jnp.float32) / KX
    freq_y = jnp.where(2 * index_y < KY, index_y, index_y - KY).astype(jnp.float32) / KY
    freq_z = jnp.where(2 * index_z < KZ, index_z, index_z - KZ).astype(jnp.float32) / KZ
    square = freq_x * freq_x + freq_y * freq_y + freq_z * freq_z
    safe = jnp.where(square > 0, square, 1.0)
    volume = float(KX * KY * KZ)
    value = jnp.exp(-math.pi**2 * safe / ewald_split**2) / (math.pi * volume * safe)
    value = value / (modulus(index_x, KX) * modulus(index_y, KY) * modulus(index_z, KZ))
    return jnp.where(square > 0, value, 0.0)


def dft_tables(length):
    index = jnp.arange(length, dtype=jnp.int32)
    angle = (index[:, None] * index[None, :] % length).astype(jnp.float32) * (
        2.0 * math.pi / length
    )
    return (jnp.cos(angle), jnp.sin(angle))


def z_slots(groups):
    planes = KZ // (2 * groups) + 1
    owner = jnp.arange(groups, dtype=jnp.int32)[:, None]
    within = jnp.arange(planes, dtype=jnp.int32)[None, :]
    ordinary = owner * (planes - 1) + within
    frequency = jnp.where(within < planes - 1, ordinary, jnp.where(owner == 0, KZ // 2, 0))
    plane_weight = jnp.where(
        within < planes - 1, jnp.where(frequency == 0, 1.0, 2.0), jnp.where(owner == 0, 1.0, 0.0)
    )
    frequency = frequency.reshape(-1)
    plane_weight = plane_weight.reshape(-1).astype(jnp.float32)
    position = jnp.arange(KZ, dtype=jnp.int32)
    angle = (frequency[:, None] * position[None, :] % KZ).astype(jnp.float32) * (2.0 * math.pi / KZ)
    usable = (plane_weight > 0).astype(jnp.float32)[:, None]
    return (planes, frequency, plane_weight, jnp.cos(angle) * usable, jnp.sin(angle) * usable)


def forward_complex(data, cos_table, sin_table, shape, axis):
    direct = jnp.dot(cos_table, data, precision=highest).reshape(shape)
    other = jnp.dot(sin_table, data, precision=highest).reshape(shape)
    real_part = jnp.take(direct, 0, axis=axis) + jnp.take(other, 1, axis=axis)
    imag_part = jnp.take(direct, 1, axis=axis) - jnp.take(other, 0, axis=axis)
    return (real_part, imag_part)


def inverse_complex(data, cos_table, sin_table, shape, axis):
    direct = jnp.dot(cos_table, data, precision=highest).reshape(shape)
    other = jnp.dot(sin_table, data, precision=highest).reshape(shape)
    real_part = jnp.take(direct, 0, axis=axis) - jnp.take(other, 1, axis=axis)
    imag_part = jnp.take(other, 0, axis=axis) + jnp.take(direct, 1, axis=axis)
    return (real_part, imag_part)


def spectrum_pen_first(grid, block_x, block_y):
    cos_x, sin_x = dft_tables(KX)
    cos_y, sin_y = dft_tables(KY)
    planes, frequency, plane_weight, cos_z, sin_z = z_slots(lax.axis_size("pen"))
    slot_total = cos_z.shape[0]
    lines = KY // lax.axis_size("grp")
    real_z = jnp.einsum("xyz,kz->ykx", grid, cos_z, precision=highest)
    imag_z = -jnp.einsum("xyz,kz->ykx", grid, sin_z, precision=highest)
    outgoing = jnp.stack([real_z, imag_z], axis=2).reshape(block_y, slot_total * 2 * block_x)
    columns = lax.all_to_all(outgoing, "pen", split_axis=1, concat_axis=0, tiled=True)
    real_y, imag_y = forward_complex(columns, cos_y, sin_y, (KY, planes, 2, block_x), 2)
    sectioned = jnp.transpose(jnp.stack([real_y, imag_y], axis=-1), (2, 0, 1, 3)).reshape(
        block_x, KY * planes * 2
    )
    rows = lax.all_to_all(sectioned, "grp", split_axis=1, concat_axis=0, tiled=True)
    real_x, imag_x = forward_complex(rows, cos_x, sin_x, (KX, lines, planes, 2), 3)
    first = lax.axis_index("pen") * planes
    index_x = jnp.arange(KX, dtype=jnp.int32)[:, None, None]
    index_y = lax.axis_index("grp") * lines + jnp.arange(lines, dtype=jnp.int32)[None, :, None]
    index_z = lax.dynamic_slice_in_dim(frequency, first, planes)[None, None, :]
    local_weight = lax.dynamic_slice_in_dim(plane_weight, first, planes)[None, None, :]
    kernel = influence(index_x, index_y, index_z)
    spectral = 0.5 * jnp.sum(local_weight * kernel * (real_x * real_x + imag_x * imag_x))
    scaled = jnp.stack([kernel * real_x, kernel * imag_x], axis=-1).reshape(KX, lines * planes * 2)
    real_b, imag_b = inverse_complex(scaled, cos_x, sin_x, (KX, lines, planes, 2), 3)
    returning = jnp.stack([real_b, imag_b], axis=-1).reshape(KX, lines * planes * 2)
    rows_home = lax.all_to_all(returning, "grp", split_axis=0, concat_axis=1, tiled=True)
    rows_home = jnp.transpose(rows_home.reshape(block_x, KY, planes, 2), (1, 2, 3, 0)).reshape(
        KY, planes * 2 * block_x
    )
    real_c, imag_c = inverse_complex(rows_home, cos_y, sin_y, (KY, planes, 2, block_x), 2)
    leaving = jnp.stack([real_c, imag_c], axis=2).reshape(KY, planes * 2 * block_x)
    home = lax.all_to_all(leaving, "pen", split_axis=0, concat_axis=1, tiled=True).reshape(
        block_y, slot_total, 2, block_x
    )
    potential = jnp.einsum(
        "ykx,kz->xyz", home[:, :, 0], plane_weight[:, None] * cos_z, precision=highest
    )
    potential = potential - jnp.einsum(
        "ykx,kz->xyz", home[:, :, 1], plane_weight[:, None] * sin_z, precision=highest
    )
    return (potential, spectral)


def local(cell_offsets, cell_z, frac, charges, tile_counts):
    groups_all, pens = lax.axis_size("grp"), lax.axis_size("pen")
    devices = groups_all * pens
    block_x = KX // groups_all
    block_y = KY // pens
    slots = charges.shape[0] // tile_counts.shape[0]
    groups = block_y // 2 * slots // (2 * LANES)
    lines = charges.shape[0] // LANES
    slot_arrays = [frac, cell_offsets, cell_z.reshape(lines, LANES), charges.reshape(lines, LANES)]
    atoms = apart([tile_counts, *slot_arrays])
    if KZ == 8 * devices and 4 * block_y == LANES and pens == 8 and block_x % 16 == 0:
        return by_halves(atoms, slots, groups, block_x, block_y)
    return by_pencils(atoms, slots, groups, block_x, block_y)


def solution(mesh):
    in_specs = (
        P(None, ("grp", "pen")),
        P(("grp", "pen")),
        P(None, ("grp", "pen")),
        P(("grp", "pen")),
        P(("grp", "pen")),
    )
    out_specs = (P(None, ("grp", "pen")), P())
    return jax.shard_map(local, mesh=mesh, in_specs=in_specs, out_specs=out_specs, check_vma=False)
```
